512 devices in a mesh: tok: 128 (over z, y, core), head: 4 (over x).
Axes of the slice: x: 4, y: 4, z: 16, core: 2. Of those that a mesh axis runs over, the one named last changes fastest.
Arguments:
- tokens: bfloat16 [32768, 2048], P('tok', 'head'), may hold values from -6 to 6
- norm_gain: float32 [2048], replicated, may hold values from 0.25 to 1.75
- w_query: bfloat16 [2048, 4096], P('tok', 'head'), may hold values from -0.125 to 0.125
- key_weight: bfloat16 [2048, 512], P('tok', 'head'), may hold values from -0.125 to 0.125
- value_weight: bfloat16 [2048, 512], P('tok', 'head'), may hold values from -0.125 to 0.125
- query_gain: float32 [128], replicated, may hold values from 0.6 to 12
- key_gain: float32 [128], replicated, may hold values from 0.6 to 12
- w_out: bfloat16 [4096, 2048], P('head', 'tok'), may hold values from -0.09375 to 0.09375
- doc_ids: int32 [32768], P('tok'), may hold values from 0 to 15, never falling along the last dimension, each value on 1 to 8192 neighbouring positions
- sentinel: int32 [32768], P('tok'), may hold values 0 or 1
- tile_reach: int32 [256], P('tok'), may hold values from 1 to 28, as said below
Outputs:
- attn_out: bfloat16 [32768, 2048], P('tok', 'head')
The draws below stay inside these ranges and needn't reach their ends.
Inputs may be any that keep to these rules, and one draw needn't show every extreme that they name: `tile_reach`: some tile's entry is 28.
All inputs are finite; a program needn't handle non-finite values. No bound on the sum of `sentinel` on one device may be relied on, other than what follows from the above.
Results may differ from the reference program's by a relative error of at most 0.014.
The reference program's roundings to bfloat16 on the way count: a program that leaves them out, or rounds other values in their place, can miss the bound.
Values may be sent and summed in bfloat16 or wider, within the bound.
No kernel may reach another device: no remote copies, remote signals or barrier semaphores. Data moves between devices by JAX's collectives and lax.ppermute only.
A program may use at most 64 MiB of HBM per device.

```python
import math
import jax
import jax.numpy as jnp
import numpy as np
from jax import lax

MODEL_WIDTH = 2048
QUERY_HEADS = 32
KEY_VALUE_HEADS = 4
HEAD_SIZE = 128
TILE_TOKENS = 128
SPAN_TILES = 28
STREAM_TOKENS = 32768
QTILES = 256
DOCS = 16
DOC_MOST = 8192
N_HEAD = 4


def draw_tile_reach(key, part):
    reach_values = jax.random.randint(key, (QTILES,), 1, SPAN_TILES + 1)
    near_spot = jax.random.randint(jax.random.fold_in(key, 11), (), 0, QTILES)
    far_spot = jax.random.randint(jax.random.fold_in(key, 7), (), 0, QTILES)
    reach_values = reach_values.at[near_spot].set(1)
    reach_values = reach_values.at[far_spot].set(SPAN_TILES)
    return reach_values.astype(jnp.int32)


def gain_values(key):
    return jax.random.uniform(key, (HEAD_SIZE,), jnp.float32, 0.6, 1.6)


def draw_query_gain(key, part):
    return gain_values(jax.random.fold_in(key, 5))


def draw_key_gain(key, part):
    return gain_values(jax.random.fold_in(key, 3))


def set_ends(entries, key, smallest, top_value):
    index_at = [jax.random.randint(jax.random.fold_in(key, axis), (), 0, length) for axis, length in enumerate(entries.shape)]
    widest = entries.shape.index(max(entries.shape))
    beside = index_at[:widest] + [(index_at[widest] + 1) % entries.shape[widest]] + index_at[widest + 1:]
    return entries.at[tuple(index_at)].set(smallest).at[tuple(beside)].set(top_value)


def level_of(key, dims, cuts, low, largest):
    level = 1.0
    for position, parts in cuts:
        draws = jax.random.uniform(jax.random.fold_in(jax.random.fold_in(key, 6), position), (parts,), jnp.float32, low / len(cuts), largest / len(cuts))
        level = level * jnp.repeat(jnp.exp(draws), dims[position] // parts).reshape((-1,) + (1,) * (len(dims) - 1 - position))
    return level


def profile(amount, total, bound, lean):
    weights = [(1 << 20) // math.isqrt(standing ** lean) + 1 for standing in range(2, amount + 1)]
    spare, given = total - bound - (amount - 1), [1] * (amount - 1)
    while spare > 0:
        candidates = [i for i in range(amount - 1) if given[i] < bound]
        mass, budget = sum([weights[i] for i in candidates]), spare
        for i in candidates:
            more = min(bound - given[i], max(1, budget * weights[i] // mass), spare)
            given[i] = given[i] + more
            spare = spare - more
    return np.array([bound] + given)


def uneven(own_key, count, total, bound, lean):
    if count == 2:
        one = jax.random.randint(own_key, (), max(1, total - bound), min(bound, total - 1) + 1)
        return jnp.stack([one, total - one])
    lengths = jnp.asarray(profile(count, total, bound, lean), jnp.int32)
    twos = (count - 1) // 2
    source_of, receiver = lengths[1:1 + 2 * twos:2], lengths[2:2 + 2 * twos:2]
    room = jnp.minimum(source_of - 1, bound - receiver)
    shifted = jax.random.randint(jax.random.fold_in(own_key, 1), (twos,), 0, 1 << 20) % (room + 1)
    lengths = lengths.at[1:1 + 2 * twos:2].set(source_of - shifted).at[2:2 + 2 * twos:2].set(receiver + shifted)
    return lengths[jax.random.permutation(jax.random.fold_in(own_key, 2), count)]


def centred(rng, extent, scale, bound, split=(), held_as=jnp.bfloat16):
    result = jax.random.normal(rng, extent, jnp.float32) * scale
    if len(split) > 0:
        result = level_of(rng, extent, split, -0.22, 0.18) * result
    return jnp.clip(result, min=-bound, max=bound).astype(held_as)


def setup_inputs(seed: int = 0) -> dict:
    streams_of = jax.random.split(jax.random.key(seed), 12)
    return {
        "tokens": centred(streams_of[0], (STREAM_TOKENS, MODEL_WIDTH), 1.0, 6.0, ((0, 128), (1, 4))),
        "norm_gain": jnp.clip(1.0 + 0.15 * jax.random.normal(streams_of[1], (MODEL_WIDTH,), jnp.float32), 0.25, 1.75),
        "w_query": centred(streams_of[2], (MODEL_WIDTH, QUERY_HEADS * HEAD_SIZE), MODEL_WIDTH ** -0.5, 0.125, ((0, 128), (1, 4))),
        "key_weight": centred(streams_of[3], (MODEL_WIDTH, KEY_VALUE_HEADS * HEAD_SIZE), MODEL_WIDTH ** -0.5, 0.125, ((0, 128), (1, 4))),
        "value_weight": centred(streams_of[4], (MODEL_WIDTH, KEY_VALUE_HEADS * HEAD_SIZE), MODEL_WIDTH ** -0.5, 0.125, ((0, 128), (1, 4))),
        "query_gain": draw_query_gain(jax.random.fold_in(streams_of[11], 71), 0),
        "key_gain": draw_key_gain(jax.random.fold_in(streams_of[11], 71), 0),
        "w_out": centred(streams_of[7], (QUERY_HEADS * HEAD_SIZE, MODEL_WIDTH), (QUERY_HEADS * HEAD_SIZE) ** -0.5, 0.09375, ((0, 4), (1, 128))),
        "doc_ids": jnp.searchsorted(jnp.cumsum(uneven(streams_of[8], DOCS, STREAM_TOKENS, DOC_MOST, 2)), jnp.arange(STREAM_TOKENS), side="right").astype(jnp.int32),
        "sentinel": set_ends((jax.random.randint(streams_of[9], (STREAM_TOKENS,), 0, 16) < 1).astype(jnp.int32), jax.random.fold_in(streams_of[9], 1), 0, 1),
        "tile_reach": draw_tile_reach(jax.random.fold_in(streams_of[11], 71), 0),
    }


EPSILON = 1e-06
THETA = 10000000.0

def rms_norm(values, gain):
    mean_square = lax.optimization_barrier(jnp.mean(values * values, axis=-1, keepdims=True))
    return values * lax.rsqrt(mean_square + EPSILON) * gain

def rotate(values, positions):
    width = values.shape[-1]
    half_width = width // 2
    freqs = THETA ** (-2.0 * jnp.arange(half_width, dtype=jnp.float32) / width)
    angles = positions[:, None] * freqs[None, :]
    cosine = jnp.cos(angles)[:, None, :]
    sine = jnp.sin(angles)[:, None, :]
    first = values[..., :half_width]
    second = values[..., half_width:]
    return jnp.concatenate([first * cosine - second * sine, second * cosine + first * sine], axis=-1)

def reference(tokens, norm_gain, w_query, key_weight, value_weight, query_gain, key_gain, w_out, doc_ids, sentinel, tile_reach):
    normalized_rows = rms_norm(tokens.astype(jnp.float32), norm_gain).astype(jnp.bfloat16)
    positions = jnp.arange(STREAM_TOKENS, dtype=jnp.int32).astype(jnp.float32)
    query_matrix = jnp.dot(normalized_rows, w_query, preferred_element_type=jnp.float32).reshape(STREAM_TOKENS, QUERY_HEADS, HEAD_SIZE)
    query_matrix = rotate(rms_norm(query_matrix, query_gain), positions).astype(jnp.bfloat16)
    complete_keys = jnp.dot(normalized_rows, key_weight, preferred_element_type=jnp.float32).reshape(STREAM_TOKENS, KEY_VALUE_HEADS, HEAD_SIZE)
    complete_keys = rotate(rms_norm(complete_keys, key_gain), positions).astype(jnp.bfloat16)
    complete_values = jnp.dot(normalized_rows, value_weight, preferred_element_type=jnp.float32).astype(jnp.bfloat16).reshape(STREAM_TOKENS, KEY_VALUE_HEADS, HEAD_SIZE)
    tags = jnp.where(sentinel == 1, 0, doc_ids + 1).astype(jnp.int32)
    border_length = SPAN_TILES * TILE_TOKENS
    window = (SPAN_TILES + 1) * TILE_TOKENS
    head_groups = QUERY_HEADS // KEY_VALUE_HEADS
    factor_scale = 1.0 / HEAD_SIZE ** 0.5
    padded_keys = jnp.concatenate([jnp.zeros((border_length, KEY_VALUE_HEADS, HEAD_SIZE), jnp.bfloat16), complete_keys], axis=0)
    padded_values = jnp.concatenate([jnp.zeros((border_length, KEY_VALUE_HEADS, HEAD_SIZE), jnp.bfloat16), complete_values], axis=0)
    tags_pad = jnp.concatenate([jnp.zeros((border_length,), jnp.int32), tags], axis=0)

    def one_tile(tile_index):
        leading_row = (tile_index * TILE_TOKENS).astype(jnp.int32)
        query_lines = lax.dynamic_slice_in_dim(query_matrix, leading_row, TILE_TOKENS, 0).reshape(TILE_TOKENS, KEY_VALUE_HEADS, head_groups, HEAD_SIZE)
        key_rows = lax.dynamic_slice_in_dim(padded_keys, leading_row, window, 0)
        value_rows = lax.dynamic_slice_in_dim(padded_values, leading_row, window, 0)
        tag_rows = lax.dynamic_slice_in_dim(tags_pad, leading_row, window, 0)
        query_docs = lax.dynamic_slice_in_dim(doc_ids, leading_row, TILE_TOKENS, 0) + 1
        query_pos = leading_row + jnp.arange(TILE_TOKENS, dtype=jnp.int32)
        key_pos = leading_row - border_length + jnp.arange(window, dtype=jnp.int32)
        lowest = tile_index - lax.dynamic_index_in_dim(tile_reach, tile_index, 0, keepdims=False)
        same_doc = (tag_rows[None, :] == query_docs[:, None]) | (key_pos[None, :] == query_pos[:, None])
        visible = same_doc & (key_pos[None, :] <= query_pos[:, None]) & (jnp.floor_divide(key_pos, TILE_TOKENS)[None, :] >= lowest)
        scores = jnp.einsum('qcgd,kcd->cgqk', query_lines.astype(jnp.float32), key_rows.astype(jnp.float32)) * factor_scale
        scores = jnp.where(visible, scores, -jnp.inf)
        peak = lax.optimization_barrier(jnp.max(scores, axis=-1, keepdims=True))
        weights = jnp.exp(scores - peak)
        weight_total = lax.optimization_barrier(jnp.sum(weights, axis=-1))
        rounded = lax.optimization_barrier(weights.astype(jnp.bfloat16)).astype(jnp.float32)
        mixed = jnp.einsum('cgqk,kcd->qcgd', rounded, value_rows.astype(jnp.float32))
        mixed = mixed / jnp.transpose(weight_total, (2, 0, 1))[..., None]
        return mixed.astype(jnp.bfloat16).reshape(TILE_TOKENS, QUERY_HEADS * HEAD_SIZE)
    attended = lax.map(one_tile, jnp.arange(QTILES, dtype=jnp.int32)).reshape(STREAM_TOKENS, QUERY_HEADS * HEAD_SIZE)
    group_cols = QUERY_HEADS * HEAD_SIZE // N_HEAD
    summed = jnp.zeros((STREAM_TOKENS, MODEL_WIDTH), jnp.float32)
    for group in range(N_HEAD):
        partial_value = jnp.dot(attended[:, group * group_cols:(group + 1) * group_cols], w_out[group * group_cols:(group + 1) * group_cols], preferred_element_type=jnp.float32)
        summed = summed + lax.optimization_barrier(partial_value.astype(jnp.bfloat16)).astype(jnp.float32)
    return summed.astype(jnp.bfloat16)
```

```python
import math

import jax
import jax.numpy as jnp
from jax import lax
from jax.experimental import pallas as pl
from jax.experimental.pallas import tpu as pltpu
from jax.sharding import Mesh, PartitionSpec as P


HEAD = 128
TILE = 128
BACK = 7
EPSILON = 1e-06
THETA = 10000000.0
TOK = ("z", "y", "core")
CHIP = ("z", "y")


def copies(shard, axis):
    count = lax.axis_size(axis)
    return lax.all_to_all(
        jnp.broadcast_to(shard[None], (count, *shard.shape)), axis, 0, 0, tiled=True
    )


def normed_and_turned(values, gain, cosine, sine):
    mean_square = jnp.mean(values * values, axis=-1, keepdims=True)
    scaled = values * lax.rsqrt(mean_square + EPSILON) * gain
    return scaled * cosine + pltpu.roll(scaled, HEAD // 2, 1) * sine


def query_kernel(x_ref, w_ref, gain_ref, cos_ref, sin_ref, out_ref, acc_ref):
    step = pl.program_id(0)

    @pl.when(step == 0)
    def _():
        acc_ref[...] = jnp.zeros_like(acc_ref)

    for half in range(2):
        rows = pl.ds(half * 256, 256)
        acc_ref[rows, :] += jnp.dot(
            x_ref[half, 0], w_ref[...], preferred_element_type=jnp.float32
        )

    @pl.when(step == pl.num_programs(0) - 1)
    def _():
        for tile in range(4):
            rows = pl.ds(tile * TILE, TILE)
            for head in range(4):
                one = acc_ref[rows, head * HEAD : (head + 1) * HEAD]
                turned = normed_and_turned(one, gain_ref[...], cos_ref[rows, :], sin_ref[rows, :])
                out_ref[tile, head] = turned.astype(jnp.bfloat16)


def project_queries(x, weights, gain, cosine, sine):
    return pl.pallas_call(
        query_kernel,
        grid=(4,),
        in_specs=[
            pl.BlockSpec((2, 1, 256, 512), lambda k: (0, k, 0, 0)),
            pl.BlockSpec((512, 512), lambda k: (k, 0)),
            pl.BlockSpec((1, HEAD), lambda k: (0, 0)),
            pl.BlockSpec((512, HEAD), lambda k: (0, 0)),
            pl.BlockSpec((512, HEAD), lambda k: (0, 0)),
        ],
        out_specs=pl.BlockSpec((4, 4, TILE, HEAD), lambda k: (0, 0, 0, 0)),
        out_shape=jax.ShapeDtypeStruct((4, 4, TILE, HEAD), jnp.bfloat16),
        scratch_shapes=[pltpu.VMEM((512, 512), jnp.float32)],
        name="project_queries",
    )(x, weights, gain, cosine, sine)


def key_value_kernel(core_ref, x_ref, w_ref, gain_ref, cos_ref, sin_ref, extra_ref, out_ref):
    is_key = core_ref[0] == 0
    for half in range(2):
        rows = pl.ds(half * 256, 256)
        total = jnp.zeros((256, HEAD), jnp.float32)
        for part in range(4):
            total += jnp.dot(
                x_ref[half, part],
                w_ref[part * 512 : (part + 1) * 512, :],
                preferred_element_type=jnp.float32,
            )
        turned = normed_and_turned(total, gain_ref[...], cos_ref[rows, :], sin_ref[rows, :])
        out_ref[rows, :] = jnp.where(is_key, turned, total).astype(jnp.bfloat16)
    out_ref[512:528, :] = extra_ref[...]


def project_keys_or_values(core, x, weights, gain, cosine, sine, extra):
    vmem = pl.BlockSpec(memory_space=pltpu.VMEM)
    return pl.pallas_call(
        key_value_kernel,
        in_specs=[pl.BlockSpec(memory_space=pltpu.SMEM)] + [vmem] * 6,
        out_specs=vmem,
        out_shape=jax.ShapeDtypeStruct((528, HEAD), jnp.bfloat16),
        name="project_keys_or_values",
    )(core, x, weights, gain, cosine, sine, extra)


def window_kernel(*refs):
    out_ref = refs[-1]
    for place, ref in enumerate(refs[:-1]):
        for core in range(2):
            out_ref[core, place] = ref[...]


def lay_window(blocks):
    vmem = pl.BlockSpec(memory_space=pltpu.VMEM)
    return pl.pallas_call(
        window_kernel,
        in_specs=[vmem] * len(blocks),
        out_specs=vmem,
        out_shape=jax.ShapeDtypeStruct((2, len(blocks), *blocks[0].shape), blocks[0].dtype),
        name="lay_window",
    )(*blocks)


def attention_kernel(q_ref, kv_ref, out_ref, tags_ref, docs_ref, m_ref, l_ref, acc_ref):
    tile = pl.program_id(0)
    lanes = lax.broadcasted_iota(jnp.int32, (1, TILE), 1)

    @pl.when(tile == 0)
    def _():
        for chip in range(BACK + 1):
            for core in range(2):
                extra = kv_ref[core, chip, 512:528, :].astype(jnp.float32)
                block = 2 * chip + core
                tags_ref[block : block + 1, :TILE] = extra[0:1]
                tags_ref[block : block + 1, TILE:] = extra[1:2]
                if chip == BACK:
                    docs_ref[core : core + 1, :] = extra[2:3]

    own_block = 2 * BACK + tile // 2
    odd = (tile % 2) == 1
    tag_row = jnp.abs(tags_ref[pl.ds(own_block, 1), :])
    doc_row = jnp.where(odd, tag_row[:, TILE:], tag_row[:, :TILE])
    diagonal = lax.broadcasted_iota(jnp.int32, (TILE, TILE), 0) == lax.broadcasted_iota(
        jnp.int32, (TILE, TILE), 1
    )
    query_doc = jnp.sum(jnp.where(diagonal, doc_row, 0.0), axis=1, keepdims=True)
    first_doc = jnp.sum(jnp.where(lanes == 0, doc_row, 0.0))
    before = jnp.sum(jnp.where(jnp.abs(tags_ref[...]) < first_doc, 1.0, 0.0)).astype(jnp.int32)
    reach_row = docs_ref[pl.ds(tile // 2, 1), :]
    reach = jnp.sum(jnp.where(lanes == tile % 2, reach_row, 0.0)).astype(jnp.int32)
    own_tile = 4 * BACK + tile
    lowest = jnp.maximum(own_tile - reach, 0)
    first_block = jnp.maximum(lowest, before // TILE) // 2

    m_ref[...] = jnp.full_like(m_ref, -1e30)
    l_ref[...] = jnp.zeros_like(l_ref)
    acc_ref[...] = jnp.zeros_like(acc_ref)
    query_pos = own_tile * TILE + lax.broadcasted_iota(jnp.int32, (TILE, 2 * TILE), 0)
    factor = math.log2(math.e) / math.sqrt(HEAD)

    def one_block(block, carry):
        chip = block // 2
        start = pl.multiple_of((block % 2) * 256, 256)
        keys = kv_ref[0, chip, pl.ds(start, 256), :]
        values = kv_ref[1, chip, pl.ds(start, 256), :]
        key_pos = block * 256 + lax.broadcasted_iota(jnp.int32, (TILE, 2 * TILE), 1)
        tags = tags_ref[pl.ds(block, 1), :]
        visible = (
            ((tags == query_doc) | (key_pos == query_pos))
            & (key_pos <= query_pos)
            & (key_pos >= lowest * TILE)
        )
        bias = jnp.where(visible, 0.0, -1e30)
        for head in range(4):
            scores = lax.dot_general(
                q_ref[0, head], keys, (((1,), (1,)), ((), ())), preferred_element_type=jnp.float32
            )
            scores = scores * factor + bias
            m_old = m_ref[head]
            peak = jnp.maximum(scores[:, :TILE], scores[:, TILE:])
            m_new = jnp.maximum(m_old, jnp.max(peak, axis=1, keepdims=True))
            shrink = jnp.exp2(m_old - m_new)
            left = jnp.exp2(scores[:, :TILE] - m_new)
            right = jnp.exp2(scores[:, TILE:] - m_new)
            m_ref[head] = m_new
            l_ref[head] = l_ref[head] * shrink + (left + right)
            weights = jnp.concatenate([left, right], axis=1).astype(jnp.bfloat16)
            mixed = jnp.dot(weights, values, preferred_element_type=jnp.float32)
            acc_ref[head] = acc_ref[head] * shrink + mixed
        return carry

    lax.fori_loop(first_block, own_block + 1, one_block, 0)
    for head in range(4):
        total = jnp.sum(l_ref[head], axis=1, keepdims=True)
        out_ref[:, head * HEAD : (head + 1) * HEAD] = (acc_ref[head] / total).astype(jnp.bfloat16)


def attend(queries, keys_values):
    return pl.pallas_call(
        attention_kernel,
        grid=(4,),
        in_specs=[
            pl.BlockSpec((1, 4, TILE, HEAD), lambda i: (i, 0, 0, 0)),
            pl.BlockSpec((2, BACK + 1, 528, HEAD), lambda i: (0, 0, 0, 0)),
        ],
        out_specs=pl.BlockSpec((TILE, 4 * HEAD), lambda i: (i, 0)),
        out_shape=jax.ShapeDtypeStruct((4 * TILE, 4 * HEAD), jnp.bfloat16),
        scratch_shapes=[
            pltpu.VMEM((2 * (BACK + 1), 2 * TILE), jnp.float32),
            pltpu.VMEM((8, TILE), jnp.float32),
            pltpu.VMEM((4, TILE, HEAD), jnp.float32),
            pltpu.VMEM((4, TILE, HEAD), jnp.float32),
            pltpu.VMEM((4, TILE, HEAD), jnp.float32),
        ],
        name="attend",
    )(queries, keys_values)


def output_kernel(core_ref, a_ref, own_ref, other_ref, out_ref):
    core = core_ref[0]
    dims = (((1,), (1,)), ((), ()))
    total = lax.dot_general(a_ref[core], own_ref[...], dims, preferred_element_type=jnp.float32)
    total += lax.dot_general(
        a_ref[1 - core], other_ref[...], dims, preferred_element_type=jnp.float32
    )
    out_ref[0] = total.astype(jnp.bfloat16)


def project_out(core, attended, gathered, other):
    return pl.pallas_call(
        output_kernel,
        grid=(4,),
        in_specs=[
            pl.BlockSpec(memory_space=pltpu.SMEM),
            pl.BlockSpec((2, 256, 512), lambda j: (0, 0, 0)),
            pl.BlockSpec((512, 512), lambda j: (j, 1)),
            pl.BlockSpec((512, 512), lambda j: (j, 0)),
        ],
        out_specs=pl.BlockSpec((1, 256, 512), lambda j: (j, 0, 0)),
        out_shape=jax.ShapeDtypeStruct((4, 256, 512), jnp.bfloat16),
        name="project_out",
    )(core, attended, gathered, other)


def layer(
    tokens,
    norm_gain,
    w_query,
    key_weight,
    value_weight,
    query_gain,
    key_gain,
    w_out,
    doc_ids,
    sentinel,
    tile_reach,
):
    core = lax.axis_index("core")
    core_arg = core.astype(jnp.int32).reshape(1)
    chip = lax.axis_index(CHIP)

    out_rows = w_out.T
    halves = [
        jnp.concatenate(
            [
                w_query[:, 512 * half : 512 * (half + 1)],
                out_rows[:, 512 * half : 512 * (half + 1)],
                (key_weight, value_weight)[half],
            ],
            axis=1,
        )
        for half in range(2)
    ]
    pieces = jnp.broadcast_to(jnp.stack(halves)[None], (4, 2, 16, 1152)).reshape(8, 16, 1152)
    plane = lax.all_to_all(pieces, ("y", "core"), 0, 0, tiled=True).reshape(128, 1152)
    wide = lax.all_gather(plane[:, :1024], "z", axis=0, tiled=True)
    narrow = lax.all_gather(plane[:, 1024:], "z", axis=0, tiled=True)

    whole = copies(tokens, "head").astype(jnp.float32)
    mean_square = jnp.mean(jnp.mean(whole * whole, axis=2, keepdims=True), axis=0, keepdims=True)
    normed = whole * lax.rsqrt(mean_square + EPSILON) * norm_gain.reshape(4, 1, 512)
    normed = copies(normed.astype(jnp.bfloat16), "core")

    positions = (chip * 512 + jnp.arange(512, dtype=jnp.int32)).astype(jnp.float32)
    freqs = THETA ** (-2.0 * jnp.arange(HEAD // 2, dtype=jnp.float32) / HEAD)
    angles = positions[:, None] * freqs[None, :]
    cosine, sine = jnp.cos(angles), jnp.sin(angles)
    cosine = jnp.concatenate([cosine, cosine], axis=1)
    sine = jnp.concatenate([-sine, sine], axis=1)

    tags = jnp.where(sentinel == 1, -(doc_ids + 1), doc_ids + 1).astype(jnp.bfloat16)
    extra = jnp.concatenate(
        [
            tags.reshape(2, TILE),
            jnp.pad(tile_reach.astype(jnp.bfloat16).reshape(1, 2), ((0, 0), (0, TILE - 2))),
            jnp.zeros((13, TILE), jnp.bfloat16),
        ]
    )
    own = project_keys_or_values(
        core_arg, normed, narrow, key_gain.reshape(1, HEAD), cosine, sine, extra
    )
    earlier = [
        lax.ppermute(own, CHIP, [(source, source + back) for source in range(64 - back)])
        for back in range(BACK, 0, -1)
    ]
    both = lay_window([*earlier, own])
    keys_values = lax.all_to_all(both, "core", 0, 0, tiled=True)

    queries = project_queries(normed, wide, query_gain.reshape(1, HEAD), cosine, sine)
    other = lax.ppermute(wide[:, 512:], "core", [(0, 1), (1, 0)])
    attended = attend(queries, keys_values)
    attended = lax.all_to_all(attended.reshape(2, 256, 512), "core", 0, 0, tiled=True)
    partials = project_out(core_arg, attended, wide, other)
    shares = lax.all_to_all(partials, "head", 0, 0, tiled=True)
    return jnp.sum(shares.astype(jnp.float32), axis=0).astype(jnp.bfloat16)


def solution(mesh):
    split = Mesh(mesh.devices.reshape(16, 4, 2, 4), ("z", "y", "core", "head"))
    return jax.shard_map(
        layer,
        mesh=split,
        in_specs=(
            P(TOK, "head"),
            P(),
            P(TOK, "head"),
            P(TOK, "head"),
            P(TOK, "head"),
            P(),
            P(),
            P("head", TOK),
            P(TOK),
            P(TOK),
            P(TOK),
        ),
        out_specs=P(TOK, "head"),
        check_vma=False,
    )
```

```python
import functools
import math

import jax
import jax.numpy as jnp
from jax import lax
from jax.experimental import pallas as pl
from jax.experimental.pallas import tpu as pltpu
from jax.sharding import Mesh, PartitionSpec as P


HEAD = 128
TILE = 128
KEYS = 512
WINDOW = 4096
BACK = 7
EPSILON = 1e-06
THETA = 10000000.0
TOK = ("z", "y", "core")
CHIP = ("z", "y")


def copies(shard, axis):
    count = lax.axis_size(axis)
    return lax.all_to_all(
        jnp.broadcast_to(shard[None], (count, *shard.shape)), axis, 0, 0, tiled=True
    )


def normed_and_turned(values, gain, cosine, sine):
    mean_square = jnp.mean(values * values, axis=-1, keepdims=True)
    scaled = values * lax.rsqrt(mean_square + EPSILON) * gain
    return scaled * cosine + pltpu.roll(scaled, HEAD // 2, 1) * sine


def query_kernel(x_ref, w_ref, gain_ref, cos_ref, sin_ref, out_ref):
    total = functools.reduce(
        jnp.add,
        [
            jnp.dot(
                x_ref[0, part],
                w_ref[part * 512 : (part + 1) * 512, :],
                preferred_element_type=jnp.float32,
            )
            for part in range(4)
        ],
    )
    for tile in range(2):
        rows = slice(tile * TILE, (tile + 1) * TILE)
        for head in range(4):
            one = total[rows, head * HEAD : (head + 1) * HEAD]
            turned = normed_and_turned(one, gain_ref[...], cos_ref[rows, :], sin_ref[rows, :])
            out_ref[tile, head] = turned.astype(jnp.bfloat16)


def project_queries(x, weights, gain, cosine, sine):
    return pl.pallas_call(
        query_kernel,
        grid=(2,),
        in_specs=[
            pl.BlockSpec((1, 4, 256, 512), lambda k: (k, 0, 0, 0)),
            pl.BlockSpec((2048, 512), lambda k: (0, 0)),
            pl.BlockSpec((1, HEAD), lambda k: (0, 0)),
            pl.BlockSpec((256, HEAD), lambda k: (k, 0)),
            pl.BlockSpec((256, HEAD), lambda k: (k, 0)),
        ],
        out_specs=pl.BlockSpec((2, 4, TILE, HEAD), lambda k: (k, 0, 0, 0)),
        out_shape=jax.ShapeDtypeStruct((4, 4, TILE, HEAD), jnp.bfloat16),
        name="project_queries",
    )(x, weights, gain, cosine, sine)


def key_value_kernel(
    core_ref, x_ref, norm_ref, w_ref, gain_ref, cos_ref, sin_ref, extra_ref, out_ref, normed_ref
):
    is_key = core_ref[0] == 0
    for half in range(2):
        rows = pl.ds(half * 256, 256)
        parts = [x_ref[half, part].astype(jnp.float32) for part in range(4)]
        squares = functools.reduce(jnp.add, [part * part for part in parts])
        mean_square = jnp.sum(squares, axis=1, keepdims=True) / 2048
        level = lax.rsqrt(mean_square + EPSILON)
        products = []
        for part in range(4):
            normed = (parts[part] * level * norm_ref[part]).astype(jnp.bfloat16)
            normed_ref[half, part] = normed
            products.append(
                jnp.dot(
                    normed,
                    w_ref[part * 512 : (part + 1) * 512, :],
                    preferred_element_type=jnp.float32,
                )
            )
        total = functools.reduce(jnp.add, products)
        turned = normed_and_turned(total, gain_ref[...], cos_ref[rows, :], sin_ref[rows, :])
        out_ref[rows, :] = jnp.where(is_key, turned, total).astype(jnp.bfloat16)
    out_ref[512:528, :] = extra_ref[...]


def project_keys_or_values(core, x, norm_gain, weights, gain, cosine, sine, extra):
    vmem = pl.BlockSpec(memory_space=pltpu.VMEM)
    return pl.pallas_call(
        key_value_kernel,
        in_specs=[pl.BlockSpec(memory_space=pltpu.SMEM)] + [vmem] * 7,
        out_specs=(vmem, vmem),
        out_shape=(
            jax.ShapeDtypeStruct((528, HEAD), jnp.bfloat16),
            jax.ShapeDtypeStruct((2, 4, 256, 512), jnp.bfloat16),
        ),
        name="project_keys_or_values",
    )(core, x, norm_gain, weights, gain, cosine, sine, extra)


def window_kernel(*refs):
    out_ref = refs[-1]
    for place, ref in enumerate(refs[:-1]):
        out_ref[512 * place : 512 * (place + 1), :] = ref[:512, :]
        out_ref[WINDOW + 16 * place : WINDOW + 16 * (place + 1), :] = ref[512:, :]


def lay_window(blocks):
    vmem = pl.BlockSpec(memory_space=pltpu.VMEM)
    return pl.pallas_call(
        window_kernel,
        in_specs=[vmem] * len(blocks),
        out_specs=vmem,
        out_shape=jax.ShapeDtypeStruct((WINDOW + 128, HEAD), jnp.bfloat16),
        name="lay_window",
    )(*blocks)


def attention_kernel(
    core_ref, q_ref, own_ref, other_ref, out_ref, kv_ref, tags_ref, reach_ref, m_ref, l_ref, acc_ref
):
    tile = pl.program_id(0)
    lanes = lax.broadcasted_iota(jnp.int32, (1, TILE), 1)

    @pl.when(tile == 0)
    def _():
        kv_ref[core_ref[0]] = own_ref[...]
        kv_ref[1 - core_ref[0]] = other_ref[...]
        for chip in range(BACK + 1):
            for core in range(2):
                row = WINDOW + 16 * chip
                extra = kv_ref[core, row : row + 16, :].astype(jnp.float32)
                place = 4 * chip + 2 * core
                tags_ref[place : place + 2, :] = extra[0:2]
                if chip == BACK:
                    reach_ref[core : core + 1, :] = extra[2:3]

    own_tile = 4 * BACK + tile
    doc_row = jnp.abs(tags_ref[pl.ds(own_tile, 1), :])
    diagonal = lax.broadcasted_iota(jnp.int32, (TILE, TILE), 0) == lax.broadcasted_iota(
        jnp.int32, (TILE, TILE), 1
    )
    query_doc = jnp.sum(jnp.where(diagonal, doc_row, 0.0), axis=1, keepdims=True)
    first_doc = jnp.sum(jnp.where(lanes == 0, doc_row, 0.0))
    before = jnp.sum(jnp.where(jnp.abs(tags_ref[...]) < first_doc, 1.0, 0.0)).astype(jnp.int32)
    reach_row = reach_ref[pl.ds(tile // 2, 1), :]
    reach = jnp.sum(jnp.where(lanes == tile % 2, reach_row, 0.0)).astype(jnp.int32)
    lowest = jnp.maximum(own_tile - reach, 0)
    first_tile = jnp.maximum(lowest, before // TILE)
    block_count = (own_tile - first_tile) // 4 + 1
    factor = math.log2(math.e) / math.sqrt(HEAD)
    query = q_ref[0].reshape(4 * TILE, HEAD)
    wide_doc = jnp.broadcast_to(query_doc, (TILE, TILE))

    def scores_of(start_tile):
        start = pl.multiple_of(start_tile * TILE, TILE)
        return lax.dot_general(
            query,
            kv_ref[0, pl.ds(start, KEYS), :],
            (((1,), (1,)), ((), ())),
            preferred_element_type=jnp.float32,
        )

    def values_of(start_tile):
        return kv_ref[1, pl.ds(pl.multiple_of(start_tile * TILE, TILE), KEYS), :]

    def tags_of(start_tile, end_tile):
        rows = []
        for place in range(4):
            inside = (start_tile + place >= lowest) & (start_tile + place < end_tile)
            rows.append(jnp.where(inside, tags_ref[pl.ds(start_tile + place, 1), :], 0.0))
        return rows

    def lay_sums(pieces, peak):
        exps = [jnp.exp2(piece * factor - peak) for piece in pieces]
        return functools.reduce(jnp.add, exps), [piece.astype(jnp.bfloat16) for piece in exps]

    start_tile = own_tile - 3
    scores = scores_of(start_tile)
    tags = tags_of(start_tile, own_tile + 1)
    key_lane = lax.broadcasted_iota(jnp.int32, (TILE, TILE), 1)
    query_row = lax.broadcasted_iota(jnp.int32, (TILE, TILE), 0)
    visible = [wide_doc == tags[place] for place in range(4)]
    visible[3] = (visible[3] & (key_lane < query_row)) | diagonal
    weights = []
    for head in range(4):
        rows = slice(head * TILE, (head + 1) * TILE)
        pieces = [
            jnp.where(visible[place], scores[rows, place * TILE : (place + 1) * TILE], -1e30)
            for place in range(4)
        ]
        peak = jnp.max(functools.reduce(jnp.maximum, pieces), axis=1, keepdims=True) * factor
        peak = jnp.broadcast_to(peak, (TILE, HEAD))
        total, exps = lay_sums(pieces, peak)
        m_ref[rows, :] = peak
        l_ref[rows, :] = total
        weights.append(jnp.concatenate(exps, axis=1))
    acc_ref[...] = jnp.dot(
        jnp.concatenate(weights, axis=0), values_of(start_tile), preferred_element_type=jnp.float32
    )

    def one_block(block, carry):
        end_tile = own_tile + 1 - 4 * block
        start_tile = jnp.maximum(end_tile - 4, 0)
        scores = scores_of(start_tile)
        tags = tags_of(start_tile, end_tile)
        visible = [wide_doc == tags[place] for place in range(4)]
        weights, shrinks = [], []
        for head in range(4):
            rows = slice(head * TILE, (head + 1) * TILE)
            pieces = [
                jnp.where(visible[place], scores[rows, place * TILE : (place + 1) * TILE], -1e30)
                for place in range(4)
            ]
            peak = jnp.max(functools.reduce(jnp.maximum, pieces), axis=1, keepdims=True) * factor
            m_old = m_ref[rows, :]
            m_new = jnp.maximum(m_old, peak)
            total, exps = lay_sums(pieces, m_new)
            shrink = jnp.exp2(m_old - m_new)
            m_ref[rows, :] = m_new
            l_ref[rows, :] = l_ref[rows, :] * shrink + total
            shrinks.append(shrink)
            weights.append(jnp.concatenate(exps, axis=1))
        mixed = jnp.dot(
            jnp.concatenate(weights, axis=0),
            values_of(start_tile),
            preferred_element_type=jnp.float32,
        )
        for head in range(4):
            rows = slice(head * TILE, (head + 1) * TILE)
            acc_ref[rows, :] = acc_ref[rows, :] * shrinks[head] + mixed[rows]
        return carry

    lax.fori_loop(1, block_count, one_block, 0)
    for head in range(4):
        rows = slice(head * TILE, (head + 1) * TILE)
        total = jnp.sum(l_ref[rows, :], axis=1, keepdims=True)
        out_ref[:, head * HEAD : (head + 1) * HEAD] = (acc_ref[rows, :] / total).astype(
            jnp.bfloat16
        )


def attend(core, queries, own, other):
    rows = WINDOW + 128
    return pl.pallas_call(
        attention_kernel,
        grid=(4,),
        in_specs=[
            pl.BlockSpec(memory_space=pltpu.SMEM),
            pl.BlockSpec((1, 4, TILE, HEAD), lambda i: (i, 0, 0, 0)),
            pl.BlockSpec((rows, HEAD), lambda i: (0, 0)),
            pl.BlockSpec((rows, HEAD), lambda i: (0, 0)),
        ],
        out_specs=pl.BlockSpec((TILE, 4 * HEAD), lambda i: (i, 0)),
        out_shape=jax.ShapeDtypeStruct((4 * TILE, 4 * HEAD), jnp.bfloat16),
        scratch_shapes=[
            pltpu.VMEM((2, rows, HEAD), jnp.bfloat16),
            pltpu.VMEM((4 * (BACK + 1), TILE), jnp.float32),
            pltpu.VMEM((8, TILE), jnp.float32),
            pltpu.VMEM((4 * TILE, HEAD), jnp.float32),
            pltpu.VMEM((4 * TILE, HEAD), jnp.float32),
            pltpu.VMEM((4 * TILE, HEAD), jnp.float32),
        ],
        name="attend",
    )(core, queries, own, other)


def output_kernel(core_ref, a_ref, own_ref, other_ref, out_ref):
    core = core_ref[0]
    dims = (((1,), (1,)), ((), ()))
    total = lax.dot_general(a_ref[core], own_ref[...], dims, preferred_element_type=jnp.float32)
    total += lax.dot_general(
        a_ref[1 - core], other_ref[...], dims, preferred_element_type=jnp.float32
    )
    out_ref[0] = total.astype(jnp.bfloat16)


def project_out(core, attended, gathered, other):
    return pl.pallas_call(
        output_kernel,
        grid=(4,),
        in_specs=[
            pl.BlockSpec(memory_space=pltpu.SMEM),
            pl.BlockSpec((2, 256, 512), lambda j: (0, 0, 0)),
            pl.BlockSpec((512, 512), lambda j: (j, 1)),
            pl.BlockSpec((512, 512), lambda j: (j, 0)),
        ],
        out_specs=pl.BlockSpec((1, 256, 512), lambda j: (j, 0, 0)),
        out_shape=jax.ShapeDtypeStruct((4, 256, 512), jnp.bfloat16),
        name="project_out",
    )(core, attended, gathered, other)


def layer(
    tokens,
    norm_gain,
    w_query,
    key_weight,
    value_weight,
    query_gain,
    key_gain,
    w_out,
    doc_ids,
    sentinel,
    tile_reach,
):
    core = lax.axis_index("core")
    core_arg = core.astype(jnp.int32).reshape(1)
    chip = lax.axis_index(CHIP)

    out_rows = w_out.T
    halves = [
        jnp.concatenate(
            [
                w_query[:, 512 * half : 512 * (half + 1)],
                out_rows[:, 512 * half : 512 * (half + 1)],
                (key_weight, value_weight)[half],
            ],
            axis=1,
        )
        for half in range(2)
    ]
    pieces = jnp.broadcast_to(jnp.stack(halves)[None], (4, 2, 16, 1152)).reshape(8, 16, 1152)
    plane = lax.all_to_all(pieces, ("y", "core"), 0, 0, tiled=True).reshape(128, 1152)
    wide = lax.all_gather(plane[:, :1024], "z", axis=0, tiled=True)
    narrow = lax.all_gather(plane[:, 1024:], "z", axis=0, tiled=True)

    whole = copies(tokens, ("core", "head")).reshape(2, 4, 256, 512)

    positions = (chip * 512 + jnp.arange(512, dtype=jnp.int32)).astype(jnp.float32)
    freqs = THETA ** (-2.0 * jnp.arange(HEAD // 2, dtype=jnp.float32) / HEAD)
    angles = positions[:, None] * freqs[None, :]
    cosine, sine = jnp.cos(angles), jnp.sin(angles)
    cosine = jnp.concatenate([cosine, cosine], axis=1)
    sine = jnp.concatenate([-sine, sine], axis=1)

    tags = jnp.where(sentinel == 1, -(doc_ids + 1), doc_ids + 1).astype(jnp.bfloat16)
    extra = jnp.concatenate(
        [
            tags.reshape(2, TILE),
            jnp.pad(tile_reach.astype(jnp.bfloat16).reshape(1, 2), ((0, 0), (0, TILE - 2))),
            jnp.zeros((13, TILE), jnp.bfloat16),
        ]
    )
    own, normed = project_keys_or_values(
        core_arg,
        whole,
        norm_gain.reshape(4, 1, 512),
        narrow,
        key_gain.reshape(1, HEAD),
        cosine,
        sine,
        extra,
    )
    earlier = [
        lax.ppermute(own, CHIP, [(source, source + back) for source in range(64 - back)])
        for back in range(BACK, 0, -1)
    ]
    window = lay_window([*earlier, own])
    window_other = lax.ppermute(window, "core", [(0, 1), (1, 0)])

    queries = project_queries(normed, wide, query_gain.reshape(1, HEAD), cosine, sine)
    other = lax.ppermute(wide[:, 512:], "core", [(0, 1), (1, 0)])
    attended = attend(core_arg, queries, window, window_other)
    attended = lax.all_to_all(attended.reshape(2, 256, 512), "core", 0, 0, tiled=True)
    partials = project_out(core_arg, attended, wide, other)
    shares = lax.all_to_all(partials, "head", 0, 0, tiled=True)
    return jnp.sum(shares.astype(jnp.float32), axis=0).astype(jnp.bfloat16)


def solution(mesh):
    split = Mesh(mesh.devices.reshape(16, 4, 2, 4), ("z", "y", "core", "head"))
    return jax.shard_map(
        layer,
        mesh=split,
        in_specs=(
            P(TOK, "head"),
            P(),
            P(TOK, "head"),
            P(TOK, "head"),
            P(TOK, "head"),
            P(),
            P(),
            P("head", TOK),
            P(TOK),
            P(TOK),
            P(TOK),
        ),
        out_specs=P(TOK, "head"),
        check_vma=False,
    )
```

```python
import functools
import math

import jax
import jax.numpy as jnp
from jax import lax
from jax.experimental import pallas as pl
from jax.experimental.pallas import tpu as pltpu
from jax.sharding import Mesh, PartitionSpec as P


HEAD = 128
TILE = 128
KEYS = 512
WINDOW = 4096
BACK = 7
EPSILON = 1e-06
THETA = 10000000.0
TOK = ("z", "y", "core")
CHIP = ("z", "y")


def copies(shard, axis):
    count = lax.axis_size(axis)
    return lax.all_to_all(
        jnp.broadcast_to(shard[None], (count, *shard.shape)), axis, 0, 0, tiled=True
    )


def normed_and_turned(values, gain, cosine, sine):
    cosine = jnp.concatenate([cosine, cosine], axis=1)
    sine = jnp.concatenate([-sine, sine], axis=1)
    mean_square = jnp.mean(values * values, axis=-1, keepdims=True)
    scaled = values * lax.rsqrt(mean_square + EPSILON) * gain
    return scaled * cosine + pltpu.roll(scaled, HEAD // 2, 1) * sine


def query_kernel(x_ref, w_ref, gain_ref, cos_ref, sin_ref, out_ref):
    total = functools.reduce(
        jnp.add,
        [
            jnp.dot(
                x_ref[0, part],
                w_ref[part * 512 : (part + 1) * 512, :],
                preferred_element_type=jnp.float32,
            )
            for part in range(4)
        ],
    )
    for tile in range(2):
        rows = slice(tile * TILE, (tile + 1) * TILE)
        for head in range(4):
            one = total[rows, head * HEAD : (head + 1) * HEAD]
            turned = normed_and_turned(one, gain_ref[...], cos_ref[rows, :], sin_ref[rows, :])
            out_ref[tile, head] = turned.astype(jnp.bfloat16)


def project_queries(x, weights, gain, cosine, sine):
    return pl.pallas_call(
        query_kernel,
        grid=(2,),
        in_specs=[
            pl.BlockSpec((1, 4, 256, 512), lambda k: (k, 0, 0, 0)),
            pl.BlockSpec((2048, 512), lambda k: (0, 0)),
            pl.BlockSpec((1, HEAD), lambda k: (0, 0)),
            pl.BlockSpec((256, HEAD // 2), lambda k: (k, 0)),
            pl.BlockSpec((256, HEAD // 2), lambda k: (k, 0)),
        ],
        out_specs=pl.BlockSpec((2, 4, TILE, HEAD), lambda k: (k, 0, 0, 0)),
        out_shape=jax.ShapeDtypeStruct((4, 4, TILE, HEAD), jnp.bfloat16),
        name="project_queries",
    )(x, weights, gain, cosine, sine)


def key_value_kernel(
    core_ref, x_ref, norm_ref, w_ref, gain_ref, cos_ref, sin_ref, extra_ref, out_ref, normed_ref
):
    is_key = core_ref[0] == 0
    for half in range(2):
        rows = pl.ds(half * 256, 256)
        parts = [x_ref[half, part].astype(jnp.float32) for part in range(4)]
        squares = functools.reduce(jnp.add, [part * part for part in parts])
        mean_square = jnp.sum(squares, axis=1, keepdims=True) / 2048
        level = lax.rsqrt(mean_square + EPSILON)
        products = []
        for part in range(4):
            normed = (parts[part] * level * norm_ref[part]).astype(jnp.bfloat16)
            normed_ref[half, part] = normed
            products.append(
                jnp.dot(
                    normed,
                    w_ref[part * 512 : (part + 1) * 512, :],
                    preferred_element_type=jnp.float32,
                )
            )
        total = functools.reduce(jnp.add, products)
        turned = normed_and_turned(total, gain_ref[...], cos_ref[rows, :], sin_ref[rows, :])
        out_ref[rows, :] = jnp.where(is_key, turned, total).astype(jnp.bfloat16)
    out_ref[512:528, :] = extra_ref[...]


def project_keys_or_values(core, x, norm_gain, weights, gain, cosine, sine, extra):
    vmem = pl.BlockSpec(memory_space=pltpu.VMEM)
    return pl.pallas_call(
        key_value_kernel,
        in_specs=[pl.BlockSpec(memory_space=pltpu.SMEM)] + [vmem] * 7,
        out_specs=(vmem, vmem),
        out_shape=(
            jax.ShapeDtypeStruct((528, HEAD), jnp.bfloat16),
            jax.ShapeDtypeStruct((2, 4, 256, 512), jnp.bfloat16),
        ),
        name="project_keys_or_values",
    )(core, x, norm_gain, weights, gain, cosine, sine, extra)


def window_kernel(*refs):
    out_ref = refs[-1]
    for place, ref in enumerate(refs[:-1]):
        out_ref[512 * place : 512 * (place + 1), :] = ref[:512, :]
        out_ref[WINDOW + 16 * place : WINDOW + 16 * (place + 1), :] = ref[512:, :]


def lay_window(blocks):
    vmem = pl.BlockSpec(memory_space=pltpu.VMEM)
    return pl.pallas_call(
        window_kernel,
        in_specs=[vmem] * len(blocks),
        out_specs=vmem,
        out_shape=jax.ShapeDtypeStruct((WINDOW + 128, HEAD), jnp.bfloat16),
        name="lay_window",
    )(*blocks)


def attention_kernel(
    core_ref, q_ref, own_ref, other_ref, out_ref, kv_ref, tags_ref, reach_ref, m_ref, l_ref, acc_ref
):
    tile = pl.program_id(0)
    lanes = lax.broadcasted_iota(jnp.int32, (1, TILE), 1)

    @pl.when(tile == 0)
    def _():
        kv_ref[core_ref[0]] = own_ref[...]
        kv_ref[1 - core_ref[0]] = other_ref[...]
        for chip in range(BACK + 1):
            for core in range(2):
                row = WINDOW + 16 * chip
                extra = kv_ref[core, row : row + 16, :].astype(jnp.float32)
                place = 4 * chip + 2 * core
                tags_ref[place : place + 2, :] = extra[0:2]
                if chip == BACK:
                    reach_ref[core : core + 1, :] = extra[2:3]

    own_tile = 4 * BACK + tile
    doc_row = jnp.abs(tags_ref[pl.ds(own_tile, 1), :])
    diagonal = lax.broadcasted_iota(jnp.int32, (TILE, TILE), 0) == lax.broadcasted_iota(
        jnp.int32, (TILE, TILE), 1
    )
    query_doc = jnp.sum(jnp.where(diagonal, doc_row, 0.0), axis=1, keepdims=True)
    first_doc = jnp.sum(jnp.where(lanes == 0, doc_row, 0.0))
    before = jnp.sum(jnp.where(jnp.abs(tags_ref[...]) < first_doc, 1.0, 0.0)).astype(jnp.int32)
    reach_row = reach_ref[pl.ds(tile // 2, 1), :]
    reach = jnp.sum(jnp.where(lanes == tile % 2, reach_row, 0.0)).astype(jnp.int32)
    lowest = jnp.maximum(own_tile - reach, 0)
    first_tile = jnp.maximum(lowest, before // TILE)
    block_count = (own_tile - first_tile) // 4 + 1
    factor = math.log2(math.e) / math.sqrt(HEAD)
    query = q_ref[0].reshape(4 * TILE, HEAD)
    wide_doc = jnp.broadcast_to(query_doc, (TILE, TILE))

    def scores_of(start_tile):
        start = pl.multiple_of(start_tile * TILE, TILE)
        return lax.dot_general(
            query,
            kv_ref[0, pl.ds(start, KEYS), :],
            (((1,), (1,)), ((), ())),
            preferred_element_type=jnp.float32,
        )

    def values_of(start_tile):
        return kv_ref[1, pl.ds(pl.multiple_of(start_tile * TILE, TILE), KEYS), :]

    def tags_of(start_tile, end_tile):
        rows = []
        for place in range(4):
            inside = (start_tile + place >= lowest) & (start_tile + place < end_tile)
            rows.append(jnp.where(inside, tags_ref[pl.ds(start_tile + place, 1), :], 0.0))
        return rows

    def lay_sums(pieces, peak):
        exps = [jnp.exp2(piece * factor - peak) for piece in pieces]
        return functools.reduce(jnp.add, exps), [piece.astype(jnp.bfloat16) for piece in exps]

    start_tile = own_tile - 3
    scores = scores_of(start_tile)
    tags = tags_of(start_tile, own_tile + 1)
    key_lane = lax.broadcasted_iota(jnp.int32, (TILE, TILE), 1)
    query_row = lax.broadcasted_iota(jnp.int32, (TILE, TILE), 0)
    visible = [wide_doc == tags[place] for place in range(4)]
    visible[3] = (visible[3] & (key_lane < query_row)) | diagonal
    weights = []
    for head in range(4):
        rows = slice(head * TILE, (head + 1) * TILE)
        pieces = [
            jnp.where(visible[place], scores[rows, place * TILE : (place + 1) * TILE], -1e30)
            for place in range(4)
        ]
        peak = jnp.max(functools.reduce(jnp.maximum, pieces), axis=1, keepdims=True) * factor
        peak = jnp.broadcast_to(peak, (TILE, HEAD))
        total, exps = lay_sums(pieces, peak)
        m_ref[rows, :] = peak
        l_ref[rows, :] = total
        weights.append(jnp.concatenate(exps, axis=1))
    acc_ref[...] = jnp.dot(
        jnp.concatenate(weights, axis=0), values_of(start_tile), preferred_element_type=jnp.float32
    )

    def one_block(block, carry):
        end_tile = own_tile + 1 - 4 * block
        start_tile = jnp.maximum(end_tile - 4, 0)
        scores = scores_of(start_tile)
        tags = tags_of(start_tile, end_tile)
        visible = [wide_doc == tags[place] for place in range(4)]
        weights, shrinks = [], []
        for head in range(4):
            rows = slice(head * TILE, (head + 1) * TILE)
            pieces = [
                jnp.where(visible[place], scores[rows, place * TILE : (place + 1) * TILE], -1e30)
                for place in range(4)
            ]
            peak = jnp.max(functools.reduce(jnp.maximum, pieces), axis=1, keepdims=True) * factor
            m_old = m_ref[rows, :]
            m_new = jnp.maximum(m_old, peak)
            total, exps = lay_sums(pieces, m_new)
            shrink = jnp.exp2(m_old - m_new)
            m_ref[rows, :] = m_new
            l_ref[rows, :] = l_ref[rows, :] * shrink + total
            shrinks.append(shrink)
            weights.append(jnp.concatenate(exps, axis=1))
        mixed = jnp.dot(
            jnp.concatenate(weights, axis=0),
            values_of(start_tile),
            preferred_element_type=jnp.float32,
        )
        for head in range(4):
            rows = slice(head * TILE, (head + 1) * TILE)
            acc_ref[rows, :] = acc_ref[rows, :] * shrinks[head] + mixed[rows]
        return carry

    lax.fori_loop(1, block_count, one_block, 0)
    for head in range(4):
        rows = slice(head * TILE, (head + 1) * TILE)
        total = jnp.sum(l_ref[rows, :], axis=1, keepdims=True)
        out_ref[:, head * HEAD : (head + 1) * HEAD] = (acc_ref[rows, :] / total).astype(
            jnp.bfloat16
        )


def attend(core, queries, own, other):
    rows = WINDOW + 128
    return pl.pallas_call(
        attention_kernel,
        grid=(4,),
        in_specs=[
            pl.BlockSpec(memory_space=pltpu.SMEM),
            pl.BlockSpec((1, 4, TILE, HEAD), lambda i: (i, 0, 0, 0)),
            pl.BlockSpec((rows, HEAD), lambda i: (0, 0)),
            pl.BlockSpec((rows, HEAD), lambda i: (0, 0)),
        ],
        out_specs=pl.BlockSpec((TILE, 4 * HEAD), lambda i: (i, 0)),
        out_shape=jax.ShapeDtypeStruct((4 * TILE, 4 * HEAD), jnp.bfloat16),
        scratch_shapes=[
            pltpu.VMEM((2, rows, HEAD), jnp.bfloat16),
            pltpu.VMEM((4 * (BACK + 1), TILE), jnp.float32),
            pltpu.VMEM((8, TILE), jnp.float32),
            pltpu.VMEM((4 * TILE, HEAD), jnp.float32),
            pltpu.VMEM((4 * TILE, HEAD), jnp.float32),
            pltpu.VMEM((4 * TILE, HEAD), jnp.float32),
        ],
        name="attend",
    )(core, queries, own, other)


def output_kernel(a_ref, w_ref, *refs):
    total = lax.dot_general(
        a_ref[...], w_ref[...], (((1,), (1,)), ((), ())), preferred_element_type=jnp.float32
    )
    if len(refs) == 2:
        total += refs[0][0].astype(jnp.float32)
    refs[-1][0] = total.astype(jnp.bfloat16)


def project_out(half, attended, weights, *shares):
    block = pl.BlockSpec((1, 256, 512), lambda j, half_ref: (j, 0, 0))
    return pl.pallas_call(
        lambda half_ref, *refs: output_kernel(*refs),
        grid_spec=pltpu.PrefetchScalarGridSpec(
            num_scalar_prefetch=1,
            grid=(4,),
            in_specs=[
                pl.BlockSpec((256, 512), lambda j, half_ref: (half_ref[0], 0)),
                pl.BlockSpec((512, 512), lambda j, half_ref: (j, 0)),
            ]
            + [block] * len(shares),
            out_specs=block,
        ),
        out_shape=jax.ShapeDtypeStruct((4, 256, 512), jnp.bfloat16),
        name="project_out",
    )(half, attended, weights, *shares)


def layer(
    tokens,
    norm_gain,
    w_query,
    key_weight,
    value_weight,
    query_gain,
    key_gain,
    w_out,
    doc_ids,
    sentinel,
    tile_reach,
):
    core = lax.axis_index("core")
    core_arg = core.astype(jnp.int32).reshape(1)
    chip = lax.axis_index(CHIP)

    out_rows = w_out.T
    halves = [
        jnp.concatenate(
            [
                w_query[:, 512 * half : 512 * (half + 1)],
                out_rows[:, 512 * half : 512 * (half + 1)],
                (key_weight, value_weight)[half],
            ],
            axis=1,
        )
        for half in range(2)
    ]
    pieces = jnp.broadcast_to(jnp.stack(halves)[None], (4, 2, 16, 1152)).reshape(8, 16, 1152)
    plane = lax.all_to_all(pieces, ("y", "core"), 0, 0, tiled=True).reshape(128, 1152)
    wide_query = lax.all_gather(plane[:, :512], "z", axis=0, tiled=True)
    wide_out = lax.all_gather(plane[:, 512:1024], "z", axis=0, tiled=True)
    narrow = lax.all_gather(plane[:, 1024:], "z", axis=0, tiled=True)

    whole = copies(tokens, ("core", "head")).reshape(2, 4, 256, 512)

    positions = (chip * 512 + jnp.arange(512, dtype=jnp.int32)).astype(jnp.float32)
    freqs = THETA ** (-2.0 * jnp.arange(HEAD // 2, dtype=jnp.float32) / HEAD)
    angles = positions[:, None] * freqs[None, :]
    cosine, sine = jnp.cos(angles), jnp.sin(angles)

    tags = jnp.where(sentinel == 1, -(doc_ids + 1), doc_ids + 1).astype(jnp.bfloat16)
    extra = jnp.concatenate(
        [
            tags.reshape(2, TILE),
            jnp.pad(tile_reach.astype(jnp.bfloat16).reshape(1, 2), ((0, 0), (0, TILE - 2))),
            jnp.zeros((13, TILE), jnp.bfloat16),
        ]
    )
    own, normed = project_keys_or_values(
        core_arg,
        whole,
        norm_gain.reshape(4, 1, 512),
        narrow,
        key_gain.reshape(1, HEAD),
        cosine,
        sine,
        extra,
    )
    earlier = []
    for back in range(BACK, 0, -1):
        steps = [(source, source + back) for source in range(64 - back)]
        earlier.append(lax.ppermute(own, CHIP, steps))
    window = lay_window([*earlier, own])
    window_other = lax.ppermute(window, "core", [(0, 1), (1, 0)])

    queries = project_queries(normed, wide_query, query_gain.reshape(1, HEAD), cosine, sine)
    attended = attend(core_arg, queries, window, window_other)
    away = project_out(1 - core_arg, attended, wide_out)
    away = lax.ppermute(away, "core", [(0, 1), (1, 0)])
    partials = project_out(core_arg, attended, wide_out, away)
    shares = lax.all_to_all(partials, "head", 0, 0, tiled=True)
    return jnp.sum(shares.astype(jnp.float32), axis=0).astype(jnp.bfloat16)


def solution(mesh):
    split = Mesh(mesh.devices.reshape(16, 4, 2, 4), ("z", "y", "core", "head"))
    return jax.shard_map(
        layer,
        mesh=split,
        in_specs=(
            P(TOK, "head"),
            P(),
            P(TOK, "head"),
            P(TOK, "head"),
            P(TOK, "head"),
            P(),
            P(),
            P("head", TOK),
            P(TOK),
            P(TOK),
            P(TOK),
        ),
        out_specs=P(TOK, "head"),
        check_vma=False,
    )
```

```python
import functools
import math

import jax
import jax.numpy as jnp
from jax import lax
from jax.experimental import pallas as pl
from jax.experimental.pallas import tpu as pltpu
from jax.sharding import Mesh, PartitionSpec as P


HEAD = 128
TILE = 128
KEYS = 512
WINDOW = 4096
BACK = 7
EPSILON = 1e-06
THETA = 10000000.0
TOK = ("z", "y", "core")
CHIP = ("z", "y")


def copies(shard, axis):
    count = lax.axis_size(axis)
    return lax.all_to_all(
        jnp.broadcast_to(shard[None], (count, *shard.shape)), axis, 0, 0, tiled=True
    )


def normed_and_turned(values, gain, cosine, sine):
    cosine = jnp.concatenate([cosine, cosine], axis=1)
    sine = jnp.concatenate([-sine, sine], axis=1)
    mean_square = jnp.mean(values * values, axis=-1, keepdims=True)
    scaled = values * lax.rsqrt(mean_square + EPSILON) * gain
    return scaled * cosine + pltpu.roll(scaled, HEAD // 2, 1) * sine


def query_kernel(x_ref, w_ref, gain_ref, cos_ref, sin_ref, out_ref):
    total = functools.reduce(
        jnp.add,
        [
            jnp.dot(
                x_ref[0, part],
                w_ref[part * 512 : (part + 1) * 512, :],
                preferred_element_type=jnp.float32,
            )
            for part in range(4)
        ],
    )
    for tile in range(2):
        rows = slice(tile * TILE, (tile + 1) * TILE)
        for head in range(4):
            one = total[rows, head * HEAD : (head + 1) * HEAD]
            turned = normed_and_turned(one, gain_ref[...], cos_ref[rows, :], sin_ref[rows, :])
            out_ref[tile, head] = turned.astype(jnp.bfloat16)


def project_queries(x, weights, gain, cosine, sine):
    return pl.pallas_call(
        query_kernel,
        grid=(2,),
        in_specs=[
            pl.BlockSpec((1, 4, 256, 512), lambda k: (k, 0, 0, 0)),
            pl.BlockSpec((2048, 512), lambda k: (0, 0)),
            pl.BlockSpec((1, HEAD), lambda k: (0, 0)),
            pl.BlockSpec((256, HEAD // 2), lambda k: (k, 0)),
            pl.BlockSpec((256, HEAD // 2), lambda k: (k, 0)),
        ],
        out_specs=pl.BlockSpec((2, 4, TILE, HEAD), lambda k: (k, 0, 0, 0)),
        out_shape=jax.ShapeDtypeStruct((4, 4, TILE, HEAD), jnp.bfloat16),
        name="project_queries",
    )(x, weights, gain, cosine, sine)


def key_value_kernel(
    core_ref, x_ref, norm_ref, w_ref, gain_ref, cos_ref, sin_ref, extra_ref, out_ref, normed_ref
):
    rows = pl.ds(pl.multiple_of(pl.program_id(0) * 256, 256), 256)
    parts = [x_ref[0, part].astype(jnp.float32) for part in range(4)]
    squares = functools.reduce(jnp.add, [part * part for part in parts])
    level = lax.rsqrt(jnp.sum(squares, axis=1, keepdims=True) / 2048 + EPSILON)
    products = []
    for part in range(4):
        normed = (parts[part] * level * norm_ref[part]).astype(jnp.bfloat16)
        normed_ref[0, part] = normed
        products.append(
            jnp.dot(
                normed,
                w_ref[part * 512 : (part + 1) * 512, :],
                preferred_element_type=jnp.float32,
            )
        )
    total = functools.reduce(jnp.add, products)
    turned = normed_and_turned(total, gain_ref[...], cos_ref[...], sin_ref[...])
    out_ref[rows, :] = jnp.where(core_ref[0] == 0, turned, total).astype(jnp.bfloat16)

    @pl.when(pl.program_id(0) == 0)
    def _():
        out_ref[512:528, :] = extra_ref[...]


def project_keys_or_values(core, x, norm_gain, weights, gain, cosine, sine, extra):
    return pl.pallas_call(
        key_value_kernel,
        grid=(2,),
        in_specs=[
            pl.BlockSpec(memory_space=pltpu.SMEM),
            pl.BlockSpec((1, 4, 256, 512), lambda k: (k, 0, 0, 0)),
            pl.BlockSpec((4, 1, 512), lambda k: (0, 0, 0)),
            pl.BlockSpec((2048, HEAD), lambda k: (0, 0)),
            pl.BlockSpec((1, HEAD), lambda k: (0, 0)),
            pl.BlockSpec((256, HEAD // 2), lambda k: (k, 0)),
            pl.BlockSpec((256, HEAD // 2), lambda k: (k, 0)),
            pl.BlockSpec((16, HEAD), lambda k: (0, 0)),
        ],
        out_specs=(
            pl.BlockSpec((528, HEAD), lambda k: (0, 0)),
            pl.BlockSpec((1, 4, 256, 512), lambda k: (k, 0, 0, 0)),
        ),
        out_shape=(
            jax.ShapeDtypeStruct((528, HEAD), jnp.bfloat16),
            jax.ShapeDtypeStruct((2, 4, 256, 512), jnp.bfloat16),
        ),
        name="project_keys_or_values",
    )(core, x, norm_gain, weights, gain, cosine, sine, extra)


def parcel_kernel(y_ref, own_ref, next_ref, far_ref, out_ref):
    for target in range(4):
        ahead = y_ref[0] <= target

        @pl.when(ahead)
        def _(target=target):
            out_ref[target, 0] = own_ref[...]
            out_ref[target, 1] = next_ref[...]

        @pl.when(jnp.logical_not(ahead))
        def _(target=target):
            out_ref[target, 0] = next_ref[...]
            out_ref[target, 1] = far_ref[...]


def parcels(y, own, next_plane, far_plane):
    vmem = pl.BlockSpec(memory_space=pltpu.VMEM)
    return pl.pallas_call(
        parcel_kernel,
        in_specs=[pl.BlockSpec(memory_space=pltpu.SMEM)] + [vmem] * 3,
        out_specs=vmem,
        out_shape=jax.ShapeDtypeStruct((4, 2, *own.shape), own.dtype),
        name="parcels",
    )(y, own, next_plane, far_plane)


def window_kernel(y_ref, parts_ref, out_ref):
    for back in range(BACK + 1):
        place = BACK - back
        source = lax.rem(y_ref[0] + 4 - back % 4, 4)
        block = parts_ref[source, back // 4]
        out_ref[512 * place : 512 * (place + 1), :] = block[:512]
        out_ref[WINDOW + 16 * place : WINDOW + 16 * (place + 1), :] = block[512:]


def lay_window(y, parts):
    vmem = pl.BlockSpec(memory_space=pltpu.VMEM)
    return pl.pallas_call(
        window_kernel,
        in_specs=[pl.BlockSpec(memory_space=pltpu.SMEM), vmem],
        out_specs=vmem,
        out_shape=jax.ShapeDtypeStruct((WINDOW + 128, HEAD), jnp.bfloat16),
        name="lay_window",
    )(y, parts)


def attention_kernel(
    core_ref,
    q_ref,
    own_ref,
    other_ref,
    w_ref,
    here_ref,
    away_ref,
    kv_ref,
    tags_ref,
    reach_ref,
    m_ref,
    l_ref,
    acc_ref,
    attended_ref,
):
    tile = pl.program_id(0)
    lanes = lax.broadcasted_iota(jnp.int32, (1, TILE), 1)

    @pl.when(tile == 0)
    def _():
        kv_ref[core_ref[0]] = own_ref[...]
        kv_ref[1 - core_ref[0]] = other_ref[...]
        for chip in range(BACK + 1):
            for core in range(2):
                row = WINDOW + 16 * chip
                extra = kv_ref[core, row : row + 16, :].astype(jnp.float32)
                place = 4 * chip + 2 * core
                tags_ref[place : place + 2, :] = extra[0:2]
                if chip == BACK:
                    reach_ref[core : core + 1, :] = extra[2:3]

    own_tile = 4 * BACK + tile
    doc_row = jnp.abs(tags_ref[pl.ds(own_tile, 1), :])
    diagonal = lax.broadcasted_iota(jnp.int32, (TILE, TILE), 0) == lax.broadcasted_iota(
        jnp.int32, (TILE, TILE), 1
    )
    query_doc = jnp.sum(jnp.where(diagonal, doc_row, 0.0), axis=1, keepdims=True)
    first_doc = jnp.sum(jnp.where(lanes == 0, doc_row, 0.0))
    before = jnp.sum(jnp.where(jnp.abs(tags_ref[...]) < first_doc, 1.0, 0.0)).astype(jnp.int32)
    reach_row = reach_ref[pl.ds(tile // 2, 1), :]
    reach = jnp.sum(jnp.where(lanes == tile % 2, reach_row, 0.0)).astype(jnp.int32)
    lowest = jnp.maximum(own_tile - reach, 0)
    first_tile = jnp.maximum(lowest, before // TILE)
    block_count = (own_tile - first_tile) // 4 + 1
    factor = math.log2(math.e) / math.sqrt(HEAD)
    query = q_ref[0].reshape(4 * TILE, HEAD)
    wide_doc = jnp.broadcast_to(query_doc, (TILE, TILE))

    def scores_of(start_tile):
        start = pl.multiple_of(start_tile * TILE, TILE)
        return lax.dot_general(
            query,
            kv_ref[0, pl.ds(start, KEYS), :],
            (((1,), (1,)), ((), ())),
            preferred_element_type=jnp.float32,
        )

    def values_of(start_tile):
        return kv_ref[1, pl.ds(pl.multiple_of(start_tile * TILE, TILE), KEYS), :]

    def tags_of(start_tile, end_tile):
        rows = []
        for place in range(4):
            inside = (start_tile + place >= lowest) & (start_tile + place < end_tile)
            rows.append(jnp.where(inside, tags_ref[pl.ds(start_tile + place, 1), :], 0.0))
        return rows

    def lay_sums(pieces, peak):
        exps = [jnp.exp2(piece * factor - peak) for piece in pieces]
        return functools.reduce(jnp.add, exps), [piece.astype(jnp.bfloat16) for piece in exps]

    start_tile = own_tile - 3
    scores = scores_of(start_tile)
    tags = tags_of(start_tile, own_tile + 1)
    key_lane = lax.broadcasted_iota(jnp.int32, (TILE, TILE), 1)
    query_row = lax.broadcasted_iota(jnp.int32, (TILE, TILE), 0)
    visible = [wide_doc == tags[place] for place in range(4)]
    visible[3] = (visible[3] & (key_lane < query_row)) | diagonal
    weights = []
    for head in range(4):
        rows = slice(head * TILE, (head + 1) * TILE)
        pieces = [
            jnp.where(visible[place], scores[rows, place * TILE : (place + 1) * TILE], -1e30)
            for place in range(4)
        ]
        peak = jnp.max(functools.reduce(jnp.maximum, pieces), axis=1, keepdims=True) * factor
        peak = jnp.broadcast_to(peak, (TILE, HEAD))
        total, exps = lay_sums(pieces, peak)
        m_ref[rows, :] = peak
        l_ref[rows, :] = total
        weights.append(jnp.concatenate(exps, axis=1))
    acc_ref[...] = jnp.dot(
        jnp.concatenate(weights, axis=0), values_of(start_tile), preferred_element_type=jnp.float32
    )

    def one_block(block, carry):
        end_tile = own_tile + 1 - 4 * block
        start_tile = jnp.maximum(end_tile - 4, 0)
        scores = scores_of(start_tile)
        tags = tags_of(start_tile, end_tile)
        visible = [wide_doc == tags[place] for place in range(4)]
        weights, shrinks = [], []
        for head in range(4):
            rows = slice(head * TILE, (head + 1) * TILE)
            pieces = [
                jnp.where(visible[place], scores[rows, place * TILE : (place + 1) * TILE], -1e30)
                for place in range(4)
            ]
            peak = jnp.max(functools.reduce(jnp.maximum, pieces), axis=1, keepdims=True) * factor
            m_old = m_ref[rows, :]
            m_new = jnp.maximum(m_old, peak)
            total, exps = lay_sums(pieces, m_new)
            shrink = jnp.exp2(m_old - m_new)
            m_ref[rows, :] = m_new
            l_ref[rows, :] = l_ref[rows, :] * shrink + total
            shrinks.append(shrink)
            weights.append(jnp.concatenate(exps, axis=1))
        mixed = jnp.dot(
            jnp.concatenate(weights, axis=0),
            values_of(start_tile),
            preferred_element_type=jnp.float32,
        )
        for head in range(4):
            rows = slice(head * TILE, (head + 1) * TILE)
            acc_ref[rows, :] = acc_ref[rows, :] * shrinks[head] + mixed[rows]
        return carry

    lax.fori_loop(1, block_count, one_block, 0)
    tile_rows = pl.ds(pl.multiple_of(tile * TILE, TILE), TILE)
    for head in range(4):
        rows = slice(head * TILE, (head + 1) * TILE)
        total = jnp.sum(l_ref[rows, :], axis=1, keepdims=True)
        attended_ref[tile_rows, head * HEAD : (head + 1) * HEAD] = (
            acc_ref[rows, :] / total
        ).astype(jnp.bfloat16)

    @pl.when(tile == 3)
    def _():
        here = pl.ds(pl.multiple_of(core_ref[0] * 256, 256), 256)
        away = pl.ds(pl.multiple_of((1 - core_ref[0]) * 256, 256), 256)
        both = jnp.concatenate([attended_ref[here, :], attended_ref[away, :]], axis=0)
        for part in range(4):
            sums = lax.dot_general(
                both,
                w_ref[part * 512 : (part + 1) * 512, :],
                (((1,), (1,)), ((), ())),
                preferred_element_type=jnp.float32,
            )
            here_ref[part] = sums[:256]
            away_ref[part] = sums[256:].astype(jnp.bfloat16)


def attend_and_project(core, queries, own, other, wide):
    rows = WINDOW + 128
    return pl.pallas_call(
        attention_kernel,
        grid=(4,),
        in_specs=[
            pl.BlockSpec(memory_space=pltpu.SMEM),
            pl.BlockSpec((1, 4, TILE, HEAD), lambda i: (i, 0, 0, 0)),
            pl.BlockSpec((rows, HEAD), lambda i: (0, 0)),
            pl.BlockSpec((rows, HEAD), lambda i: (0, 0)),
            pl.BlockSpec((2048, 512), lambda i: (0, 1)),
        ],
        out_specs=(
            pl.BlockSpec((4, 256, 512), lambda i: (0, 0, 0)),
            pl.BlockSpec((4, 256, 512), lambda i: (0, 0, 0)),
        ),
        out_shape=(
            jax.ShapeDtypeStruct((4, 256, 512), jnp.float32),
            jax.ShapeDtypeStruct((4, 256, 512), jnp.bfloat16),
        ),
        scratch_shapes=[
            pltpu.VMEM((2, rows, HEAD), jnp.bfloat16),
            pltpu.VMEM((4 * (BACK + 1), TILE), jnp.float32),
            pltpu.VMEM((8, TILE), jnp.float32),
            pltpu.VMEM((4 * TILE, HEAD), jnp.float32),
            pltpu.VMEM((4 * TILE, HEAD), jnp.float32),
            pltpu.VMEM((4 * TILE, HEAD), jnp.float32),
            pltpu.VMEM((4 * TILE, 4 * HEAD), jnp.bfloat16),
        ],
        name="attend_and_project",
    )(core, queries, own, other, wide)


def layer(
    tokens,
    norm_gain,
    w_query,
    key_weight,
    value_weight,
    query_gain,
    key_gain,
    w_out,
    doc_ids,
    sentinel,
    tile_reach,
):
    core = lax.axis_index("core")
    core_arg = core.astype(jnp.int32).reshape(1)
    chip = lax.axis_index(CHIP)

    out_rows = w_out.T
    halves = [
        jnp.concatenate(
            [
                w_query[:, 512 * half : 512 * (half + 1)],
                out_rows[:, 512 * half : 512 * (half + 1)],
                (key_weight, value_weight)[half],
            ],
            axis=1,
        )
        for half in range(2)
    ]
    pieces = jnp.broadcast_to(jnp.stack(halves)[None], (4, 2, 16, 1152)).reshape(8, 16, 1152)
    plane = lax.all_to_all(pieces, ("y", "core"), 0, 0, tiled=True).reshape(128, 1152)
    wide = lax.all_gather(plane[:, :1024], "z", axis=0, tiled=True)
    narrow = lax.all_gather(plane[:, 1024:], "z", axis=0, tiled=True)

    whole = copies(tokens, ("core", "head")).reshape(2, 4, 256, 512)

    positions = (chip * 512 + jnp.arange(512, dtype=jnp.int32)).astype(jnp.float32)
    freqs = THETA ** (-2.0 * jnp.arange(HEAD // 2, dtype=jnp.float32) / HEAD)
    angles = positions[:, None] * freqs[None, :]
    cosine, sine = jnp.cos(angles), jnp.sin(angles)

    tags = jnp.where(sentinel == 1, -(doc_ids + 1), doc_ids + 1).astype(jnp.bfloat16)
    extra = jnp.concatenate(
        [
            tags.reshape(2, TILE),
            jnp.pad(tile_reach.astype(jnp.bfloat16).reshape(1, 2), ((0, 0), (0, TILE - 2))),
            jnp.zeros((13, TILE), jnp.bfloat16),
        ]
    )
    own, normed = project_keys_or_values(
        core_arg,
        whole,
        norm_gain.reshape(4, 1, 512),
        narrow,
        key_gain.reshape(1, HEAD),
        cosine,
        sine,
        extra,
    )
    y_arg = lax.axis_index("y").astype(jnp.int32).reshape(1)
    next_plane, far_plane = (
        lax.ppermute(own, "z", [(source, source + step) for source in range(16 - step)])
        for step in (1, 2)
    )
    parts = parcels(y_arg, own, next_plane, far_plane)
    parts = lax.all_to_all(parts, "y", 0, 0, tiled=True)
    window = lay_window(y_arg, parts)
    window_other = lax.ppermute(window, "core", [(0, 1), (1, 0)])
    queries = project_queries(normed, wide, query_gain.reshape(1, HEAD), cosine, sine)
    here, away = attend_and_project(core_arg, queries, window, window_other, wide)
    away = lax.ppermute(away, "core", [(0, 1), (1, 0)])
    partials = (here + away.astype(jnp.float32)).astype(jnp.bfloat16)
    shares = lax.all_to_all(partials, "head", 0, 0, tiled=True)
    return jnp.sum(shares.astype(jnp.float32), axis=0).astype(jnp.bfloat16)


def solution(mesh):
    split = Mesh(mesh.devices.reshape(16, 4, 2, 4), ("z", "y", "core", "head"))
    return jax.shard_map(
        layer,
        mesh=split,
        in_specs=(
            P(TOK, "head"),
            P(),
            P(TOK, "head"),
            P(TOK, "head"),
            P(TOK, "head"),
            P(),
            P(),
            P("head", TOK),
            P(TOK),
            P(TOK),
            P(TOK),
        ),
        out_specs=P(TOK, "head"),
        check_vma=False,
    )
```

```python
import functools
import math

import jax
import jax.numpy as jnp
from jax import lax
from jax.experimental import pallas as pl
from jax.experimental.pallas import tpu as pltpu
from jax.sharding import Mesh, PartitionSpec as P


HEAD = 128
TILE = 128
KEYS = 512
WINDOW = 4096
BACK = 7
EPSILON = 1e-06
THETA = 10000000.0
TOK = ("z", "y", "core")
CHIP = ("z", "y")


def grant(mebibytes):
    return pltpu.CompilerParams(vmem_limit_bytes=mebibytes << 20)


def copies(shard, axis):
    count = lax.axis_size(axis)
    return lax.all_to_all(
        jnp.broadcast_to(shard[None], (count, *shard.shape)), axis, 0, 0, tiled=True
    )


def normed_and_turned(values, gain, cosine, sine):
    cosine = jnp.concatenate([cosine, cosine], axis=1)
    sine = jnp.concatenate([-sine, sine], axis=1)
    mean_square = jnp.mean(values * values, axis=-1, keepdims=True)
    scaled = values * lax.rsqrt(mean_square + EPSILON) * gain
    return scaled * cosine + pltpu.roll(scaled, HEAD // 2, 1) * sine


def query_kernel(x_ref, w_ref, gain_ref, cos_ref, sin_ref, out_ref):
    total = functools.reduce(
        jnp.add,
        [
            jnp.dot(
                x_ref[0, part],
                w_ref[part * 512 : (part + 1) * 512, :],
                preferred_element_type=jnp.float32,
            )
            for part in range(4)
        ],
    )
    for tile in range(2):
        rows = slice(tile * TILE, (tile + 1) * TILE)
        for head in range(4):
            one = total[rows, head * HEAD : (head + 1) * HEAD]
            turned = normed_and_turned(one, gain_ref[...], cos_ref[rows, :], sin_ref[rows, :])
            out_ref[tile, head] = turned.astype(jnp.bfloat16)


def project_queries(x, weights, gain, cosine, sine):
    return pl.pallas_call(
        query_kernel,
        grid=(2,),
        in_specs=[
            pl.BlockSpec((1, 4, 256, 512), lambda k: (k, 0, 0, 0)),
            pl.BlockSpec((2048, 512), lambda k: (0, 0)),
            pl.BlockSpec((1, HEAD), lambda k: (0, 0)),
            pl.BlockSpec((256, HEAD // 2), lambda k: (k, 0)),
            pl.BlockSpec((256, HEAD // 2), lambda k: (k, 0)),
        ],
        out_specs=pl.BlockSpec((2, 4, TILE, HEAD), lambda k: (k, 0, 0, 0)),
        out_shape=jax.ShapeDtypeStruct((4, 4, TILE, HEAD), jnp.bfloat16),
        compiler_params=grant(16),
        name="project_queries",
    )(x, weights, gain, cosine, sine)


def key_value_kernel(
    core_ref, x_ref, norm_ref, w_ref, gain_ref, cos_ref, sin_ref, extra_ref, out_ref, normed_ref
):
    rows = pl.ds(pl.multiple_of(pl.program_id(0) * 256, 256), 256)
    parts = [x_ref[0, part].astype(jnp.float32) for part in range(4)]
    squares = functools.reduce(jnp.add, [part * part for part in parts])
    level = lax.rsqrt(jnp.sum(squares, axis=1, keepdims=True) / 2048 + EPSILON)
    products = []
    for part in range(4):
        normed = (parts[part] * level * norm_ref[part]).astype(jnp.bfloat16)
        normed_ref[0, part] = normed
        products.append(
            jnp.dot(
                normed,
                w_ref[part * 512 : (part + 1) * 512, :],
                preferred_element_type=jnp.float32,
            )
        )
    total = functools.reduce(jnp.add, products)
    turned = normed_and_turned(total, gain_ref[...], cos_ref[...], sin_ref[...])
    out_ref[rows, :] = jnp.where(core_ref[0] == 0, turned, total).astype(jnp.bfloat16)

    @pl.when(pl.program_id(0) == 0)
    def _():
        out_ref[512:528, :] = extra_ref[...]


def project_keys_or_values(core, x, norm_gain, weights, gain, cosine, sine, extra):
    return pl.pallas_call(
        key_value_kernel,
        grid=(2,),
        in_specs=[
            pl.BlockSpec(memory_space=pltpu.SMEM),
            pl.BlockSpec((1, 4, 256, 512), lambda k: (k, 0, 0, 0)),
            pl.BlockSpec((4, 1, 512), lambda k: (0, 0, 0)),
            pl.BlockSpec((2048, HEAD), lambda k: (0, 0)),
            pl.BlockSpec((1, HEAD), lambda k: (0, 0)),
            pl.BlockSpec((256, HEAD // 2), lambda k: (k, 0)),
            pl.BlockSpec((256, HEAD // 2), lambda k: (k, 0)),
            pl.BlockSpec((16, HEAD), lambda k: (0, 0)),
        ],
        out_specs=(
            pl.BlockSpec((528, HEAD), lambda k: (0, 0)),
            pl.BlockSpec((1, 4, 256, 512), lambda k: (k, 0, 0, 0)),
        ),
        out_shape=(
            jax.ShapeDtypeStruct((528, HEAD), jnp.bfloat16),
            jax.ShapeDtypeStruct((2, 4, 256, 512), jnp.bfloat16),
        ),
        compiler_params=grant(12),
        name="project_keys_or_values",
    )(core, x, norm_gain, weights, gain, cosine, sine, extra)


def parcel_kernel(y_ref, own_ref, next_ref, far_ref, out_ref):
    for target in range(4):
        ahead = y_ref[0] <= target

        @pl.when(ahead)
        def _(target=target):
            out_ref[target, 0] = own_ref[...]
            out_ref[target, 1] = next_ref[...]

        @pl.when(jnp.logical_not(ahead))
        def _(target=target):
            out_ref[target, 0] = next_ref[...]
            out_ref[target, 1] = far_ref[...]


def parcels(y, own, next_plane, far_plane):
    vmem = pl.BlockSpec(memory_space=pltpu.VMEM)
    return pl.pallas_call(
        parcel_kernel,
        in_specs=[pl.BlockSpec(memory_space=pltpu.SMEM)] + [vmem] * 3,
        out_specs=vmem,
        out_shape=jax.ShapeDtypeStruct((4, 2, *own.shape), own.dtype),
        compiler_params=grant(4),
        name="parcels",
    )(y, own, next_plane, far_plane)


def window_kernel(y_ref, parts_ref, out_ref):
    for back in range(BACK + 1):
        place = BACK - back
        source = lax.rem(y_ref[0] + 4 - back % 4, 4)
        block = parts_ref[source, back // 4]
        out_ref[512 * place : 512 * (place + 1), :] = block[:512]
        out_ref[WINDOW + 16 * place : WINDOW + 16 * (place + 1), :] = block[512:]


def lay_window(y, parts):
    vmem = pl.BlockSpec(memory_space=pltpu.VMEM)
    return pl.pallas_call(
        window_kernel,
        in_specs=[pl.BlockSpec(memory_space=pltpu.SMEM), vmem],
        out_specs=vmem,
        out_shape=jax.ShapeDtypeStruct((WINDOW + 128, HEAD), jnp.bfloat16),
        compiler_params=grant(4),
        name="lay_window",
    )(y, parts)


def attention_kernel(
    core_ref,
    q_ref,
    own_ref,
    other_ref,
    w_ref,
    here_ref,
    away_ref,
    kv_ref,
    tags_ref,
    reach_ref,
    m_ref,
    l_ref,
    acc_ref,
    attended_ref,
):
    tile = pl.program_id(0)
    lanes = lax.broadcasted_iota(jnp.int32, (1, TILE), 1)

    @pl.when(tile == 0)
    def _():
        kv_ref[core_ref[0]] = own_ref[...]
        kv_ref[1 - core_ref[0]] = other_ref[...]
        for chip in range(BACK + 1):
            for core in range(2):
                row = WINDOW + 16 * chip
                extra = kv_ref[core, row : row + 16, :].astype(jnp.float32)
                place = 4 * chip + 2 * core
                tags_ref[place : place + 2, :] = extra[0:2]
                if chip == BACK:
                    reach_ref[core : core + 1, :] = extra[2:3]

    own_tile = 4 * BACK + tile
    doc_row = jnp.abs(tags_ref[pl.ds(own_tile, 1), :])
    diagonal = lax.broadcasted_iota(jnp.int32, (TILE, TILE), 0) == lax.broadcasted_iota(
        jnp.int32, (TILE, TILE), 1
    )
    query_doc = jnp.sum(jnp.where(diagonal, doc_row, 0.0), axis=1, keepdims=True)
    first_doc = jnp.sum(jnp.where(lanes == 0, doc_row, 0.0))
    before = jnp.sum(jnp.where(jnp.abs(tags_ref[...]) < first_doc, 1.0, 0.0)).astype(jnp.int32)
    reach_row = reach_ref[pl.ds(tile // 2, 1), :]
    reach = jnp.sum(jnp.where(lanes == tile % 2, reach_row, 0.0)).astype(jnp.int32)
    lowest = jnp.maximum(own_tile - reach, 0)
    first_tile = jnp.maximum(lowest, before // TILE)
    block_count = (own_tile - first_tile) // 4 + 1
    factor = math.log2(math.e) / math.sqrt(HEAD)
    query = q_ref[0].reshape(4 * TILE, HEAD)
    wide_doc = jnp.broadcast_to(query_doc, (TILE, TILE))

    def scores_of(start_tile):
        start = pl.multiple_of(start_tile * TILE, TILE)
        return lax.dot_general(
            query,
            kv_ref[0, pl.ds(start, KEYS), :],
            (((1,), (1,)), ((), ())),
            preferred_element_type=jnp.float32,
        )

    def values_of(start_tile):
        return kv_ref[1, pl.ds(pl.multiple_of(start_tile * TILE, TILE), KEYS), :]

    def tags_of(start_tile, end_tile):
        rows = []
        for place in range(4):
            inside = (start_tile + place >= lowest) & (start_tile + place < end_tile)
            rows.append(jnp.where(inside, tags_ref[pl.ds(start_tile + place, 1), :], 0.0))
        return rows

    def lay_sums(pieces, peak):
        exps = [jnp.exp2(piece * factor - peak) for piece in pieces]
        return functools.reduce(jnp.add, exps), [piece.astype(jnp.bfloat16) for piece in exps]

    start_tile = own_tile - 3
    scores = scores_of(start_tile)
    tags = tags_of(start_tile, own_tile + 1)
    key_lane = lax.broadcasted_iota(jnp.int32, (TILE, TILE), 1)
    query_row = lax.broadcasted_iota(jnp.int32, (TILE, TILE), 0)
    visible = [wide_doc == tags[place] for place in range(4)]
    visible[3] = (visible[3] & (key_lane < query_row)) | diagonal
    weights = []
    for head in range(4):
        rows = slice(head * TILE, (head + 1) * TILE)
        pieces = [
            jnp.where(visible[place], scores[rows, place * TILE : (place + 1) * TILE], -1e30)
            for place in range(4)
        ]
        peak = jnp.max(functools.reduce(jnp.maximum, pieces), axis=1, keepdims=True) * factor
        peak = jnp.broadcast_to(peak, (TILE, HEAD))
        total, exps = lay_sums(pieces, peak)
        m_ref[rows, :] = peak
        l_ref[rows, :] = total
        weights.append(jnp.concatenate(exps, axis=1))
    acc_ref[...] = jnp.dot(
        jnp.concatenate(weights, axis=0), values_of(start_tile), preferred_element_type=jnp.float32
    )

    def one_block(block, carry):
        end_tile = own_tile + 1 - 4 * block
        start_tile = jnp.maximum(end_tile - 4, 0)
        scores = scores_of(start_tile)
        tags = tags_of(start_tile, end_tile)
        visible = [wide_doc == tags[place] for place in range(4)]
        weights, shrinks = [], []
        for head in range(4):
            rows = slice(head * TILE, (head + 1) * TILE)
            pieces = [
                jnp.where(visible[place], scores[rows, place * TILE : (place + 1) * TILE], -1e30)
                for place in range(4)
            ]
            peak = jnp.max(functools.reduce(jnp.maximum, pieces), axis=1, keepdims=True) * factor
            m_old = m_ref[rows, :]
            m_new = jnp.maximum(m_old, peak)
            total, exps = lay_sums(pieces, m_new)
            shrink = jnp.exp2(m_old - m_new)
            m_ref[rows, :] = m_new
            l_ref[rows, :] = l_ref[rows, :] * shrink + total
            shrinks.append(shrink)
            weights.append(jnp.concatenate(exps, axis=1))
        mixed = jnp.dot(
            jnp.concatenate(weights, axis=0),
            values_of(start_tile),
            preferred_element_type=jnp.float32,
        )
        for head in range(4):
            rows = slice(head * TILE, (head + 1) * TILE)
            acc_ref[rows, :] = acc_ref[rows, :] * shrinks[head] + mixed[rows]
        return carry

    lax.fori_loop(1, block_count, one_block, 0)
    tile_rows = pl.ds(pl.multiple_of(tile * TILE, TILE), TILE)
    for head in range(4):
        rows = slice(head * TILE, (head + 1) * TILE)
        total = jnp.sum(l_ref[rows, :], axis=1, keepdims=True)
        attended_ref[tile_rows, head * HEAD : (head + 1) * HEAD] = (
            acc_ref[rows, :] / total
        ).astype(jnp.bfloat16)

    @pl.when(tile == 3)
    def _():
        here = pl.ds(pl.multiple_of(core_ref[0] * 256, 256), 256)
        away = pl.ds(pl.multiple_of((1 - core_ref[0]) * 256, 256), 256)
        both = jnp.concatenate([attended_ref[here, :], attended_ref[away, :]], axis=0)
        for part in range(4):
            sums = lax.dot_general(
                both,
                w_ref[part * 512 : (part + 1) * 512, :],
                (((1,), (1,)), ((), ())),
                preferred_element_type=jnp.float32,
            )
            here_ref[part] = sums[:256]
            away_ref[part] = sums[256:].astype(jnp.bfloat16)


def attend_and_project(core, queries, own, other, wide):
    rows = WINDOW + 128
    return pl.pallas_call(
        attention_kernel,
        grid=(4,),
        in_specs=[
            pl.BlockSpec(memory_space=pltpu.SMEM),
            pl.BlockSpec((1, 4, TILE, HEAD), lambda i: (i, 0, 0, 0)),
            pl.BlockSpec((rows, HEAD), lambda i: (0, 0)),
            pl.BlockSpec((rows, HEAD), lambda i: (0, 0)),
            pl.BlockSpec((2048, 512), lambda i: (0, 1)),
        ],
        out_specs=(
            pl.BlockSpec((4, 256, 512), lambda i: (0, 0, 0)),
            pl.BlockSpec((4, 256, 512), lambda i: (0, 0, 0)),
        ),
        out_shape=(
            jax.ShapeDtypeStruct((4, 256, 512), jnp.float32),
            jax.ShapeDtypeStruct((4, 256, 512), jnp.bfloat16),
        ),
        scratch_shapes=[
            pltpu.VMEM((2, rows, HEAD), jnp.bfloat16),
            pltpu.VMEM((4 * (BACK + 1), TILE), jnp.float32),
            pltpu.VMEM((8, TILE), jnp.float32),
            pltpu.VMEM((4 * TILE, HEAD), jnp.float32),
            pltpu.VMEM((4 * TILE, HEAD), jnp.float32),
            pltpu.VMEM((4 * TILE, HEAD), jnp.float32),
            pltpu.VMEM((4 * TILE, 4 * HEAD), jnp.bfloat16),
        ],
        compiler_params=grant(26),
        name="attend_and_project",
    )(core, queries, own, other, wide)


def layer(
    tokens,
    norm_gain,
    w_query,
    key_weight,
    value_weight,
    query_gain,
    key_gain,
    w_out,
    doc_ids,
    sentinel,
    tile_reach,
):
    core = lax.axis_index("core")
    core_arg = core.astype(jnp.int32).reshape(1)
    chip = lax.axis_index(CHIP)

    out_rows = w_out.T
    halves = [
        jnp.concatenate(
            [
                w_query[:, 512 * half : 512 * (half + 1)],
                out_rows[:, 512 * half : 512 * (half + 1)],
                (key_weight, value_weight)[half],
            ],
            axis=1,
        )
        for half in range(2)
    ]
    pieces = jnp.broadcast_to(jnp.stack(halves)[None], (4, 2, 16, 1152)).reshape(8, 16, 1152)
    plane = lax.all_to_all(pieces, ("y", "core"), 0, 0, tiled=True).reshape(128, 1152)
    wide = lax.all_gather(plane[:, :1024], "z", axis=0, tiled=True)
    narrow = lax.all_gather(plane[:, 1024:], "z", axis=0, tiled=True)

    whole = copies(tokens, ("core", "head")).reshape(2, 4, 256, 512)

    positions = (chip * 512 + jnp.arange(512, dtype=jnp.int32)).astype(jnp.float32)
    freqs = THETA ** (-2.0 * jnp.arange(HEAD // 2, dtype=jnp.float32) / HEAD)
    angles = positions[:, None] * freqs[None, :]
    cosine, sine = jnp.cos(angles), jnp.sin(angles)

    tags = jnp.where(sentinel == 1, -(doc_ids + 1), doc_ids + 1).astype(jnp.bfloat16)
    extra = jnp.concatenate(
        [
            tags.reshape(2, TILE),
            jnp.pad(tile_reach.astype(jnp.bfloat16).reshape(1, 2), ((0, 0), (0, TILE - 2))),
            jnp.zeros((13, TILE), jnp.bfloat16),
        ]
    )
    own, normed = project_keys_or_values(
        core_arg,
        whole,
        norm_gain.reshape(4, 1, 512),
        narrow,
        key_gain.reshape(1, HEAD),
        cosine,
        sine,
        extra,
    )
    y_arg = lax.axis_index("y").astype(jnp.int32).reshape(1)
    next_plane, far_plane = (
        lax.ppermute(own, "z", [(source, source + step) for source in range(16 - step)])
        for step in (1, 2)
    )
    parts = parcels(y_arg, own, next_plane, far_plane)
    parts = lax.all_to_all(parts, "y", 0, 0, tiled=True)
    window = lay_window(y_arg, parts)
    window_other = lax.ppermute(window, "core", [(0, 1), (1, 0)])
    queries = project_queries(
        pltpu.with_memory_space_constraint(normed, pltpu.HBM),
        pltpu.with_memory_space_constraint(wide, pltpu.HBM),
        query_gain.reshape(1, HEAD),
        cosine,
        sine,
    )
    window_other = pltpu.with_memory_space_constraint(window_other, pltpu.VMEM)
    here, away = attend_and_project(core_arg, queries, window, window_other, wide)
    away = lax.ppermute(away, "core", [(0, 1), (1, 0)])
    partials = (here + away.astype(jnp.float32)).astype(jnp.bfloat16)
    shares = lax.all_to_all(partials, "head", 0, 0, tiled=True)
    return jnp.sum(shares.astype(jnp.float32), axis=0).astype(jnp.bfloat16)


def solution(mesh):
    split = Mesh(mesh.devices.reshape(16, 4, 2, 4), ("z", "y", "core", "head"))
    return jax.shard_map(
        layer,
        mesh=split,
        in_specs=(
            P(TOK, "head"),
            P(),
            P(TOK, "head"),
            P(TOK, "head"),
            P(TOK, "head"),
            P(),
            P(),
            P("head", TOK),
            P(TOK),
            P(TOK),
            P(TOK),
        ),
        out_specs=P(TOK, "head"),
        check_vma=False,
    )
```

```python
import functools
import math

import jax
import jax.numpy as jnp
from jax import lax
from jax.experimental import pallas as pl
from jax.experimental.pallas import tpu as pltpu
from jax.sharding import Mesh, PartitionSpec as P


HEAD = 128
TILE = 128
KEYS = 512
WINDOW = 4096
BACK = 7
EPSILON = 1e-06
THETA = 10000000.0
TOK = ("z", "y", "core")
CHIP = ("z", "y")


def grant(mebibytes):
    return pltpu.CompilerParams(vmem_limit_bytes=mebibytes << 20)


def off_chip(array):
    return pltpu.with_memory_space_constraint(array, pltpu.HBM)


def copies(shard, axis):
    count = lax.axis_size(axis)
    return lax.all_to_all(
        jnp.broadcast_to(shard[None], (count, *shard.shape)), axis, 0, 0, tiled=True
    )


def pieces_kernel(query_ref, out_ref_rows, key_ref, value_ref, pieces_ref):
    for y in range(4):
        for half in range(2):
            columns = slice(512 * half, 512 * (half + 1))
            pieces_ref[y, half, :, :512] = query_ref[:, columns]
            pieces_ref[y, half, :, 512:1024] = out_ref_rows[:, columns]
            pieces_ref[y, half, :, 1024:] = (key_ref, value_ref)[half][...]


def lay_pieces(query_rows, out_rows, key_rows, value_rows):
    vmem = pl.BlockSpec(memory_space=pltpu.VMEM)
    return pl.pallas_call(
        pieces_kernel,
        in_specs=[vmem] * 4,
        out_specs=vmem,
        out_shape=pltpu.VMEM((4, 2, 16, 1152), jnp.bfloat16),
        compiler_params=grant(4),
        name="lay_pieces",
    )(query_rows, out_rows, key_rows, value_rows)


def normed_and_turned(values, gain, cosine, sine):
    cosine = jnp.concatenate([cosine, cosine], axis=1)
    sine = jnp.concatenate([-sine, sine], axis=1)
    mean_square = jnp.mean(values * values, axis=-1, keepdims=True)
    scaled = values * lax.rsqrt(mean_square + EPSILON) * gain
    return scaled * cosine + pltpu.roll(scaled, HEAD // 2, 1) * sine


def query_part(total, q_ref, half, gain, cos_ref, sin_ref):
    for tile in range(2):
        rows = slice(tile * TILE, (tile + 1) * TILE)
        place = slice((2 * half + tile) * TILE, (2 * half + tile + 1) * TILE)
        for head in range(4):
            one = total[rows, head * HEAD : (head + 1) * HEAD]
            turned = normed_and_turned(one, gain, cos_ref[place, :], sin_ref[place, :])
            q_ref[2 * half + tile, head] = turned.astype(jnp.bfloat16)


def key_value_kernel(
    core_ref, x_ref, norm_ref, w_ref, gain_ref, cos_ref, sin_ref, extra_ref, out_ref, normed_ref
):
    rows = pl.ds(pl.multiple_of(pl.program_id(0) * 256, 256), 256)
    parts = [x_ref[0, part].astype(jnp.float32) for part in range(4)]
    squares = functools.reduce(jnp.add, [part * part for part in parts])
    level = lax.rsqrt(jnp.sum(squares, axis=1, keepdims=True) / 2048 + EPSILON)
    products = []
    for part in range(4):
        normed = (parts[part] * level * norm_ref[part]).astype(jnp.bfloat16)
        normed_ref[0, part] = normed
        products.append(
            jnp.dot(
                normed,
                w_ref[part * 512 : (part + 1) * 512, :],
                preferred_element_type=jnp.float32,
            )
        )
    total = functools.reduce(jnp.add, products)
    turned = normed_and_turned(total, gain_ref[...], cos_ref[...], sin_ref[...])
    out_ref[rows, :] = jnp.where(core_ref[0] == 0, turned, total).astype(jnp.bfloat16)

    @pl.when(pl.program_id(0) == 0)
    def _():
        out_ref[512:528, :] = extra_ref[...]


def project_keys_or_values(core, x, norm_gain, weights, gain, cosine, sine, extra):
    return pl.pallas_call(
        key_value_kernel,
        grid=(2,),
        in_specs=[
            pl.BlockSpec(memory_space=pltpu.SMEM),
            pl.BlockSpec((1, 4, 256, 512), lambda k: (k, 0, 0, 0)),
            pl.BlockSpec((4, 1, 512), lambda k: (0, 0, 0)),
            pl.BlockSpec((2048, HEAD), lambda k: (0, 0)),
            pl.BlockSpec((1, HEAD), lambda k: (0, 0)),
            pl.BlockSpec((256, HEAD // 2), lambda k: (k, 0)),
            pl.BlockSpec((256, HEAD // 2), lambda k: (k, 0)),
            pl.BlockSpec((16, HEAD), lambda k: (0, 0)),
        ],
        out_specs=(
            pl.BlockSpec((528, HEAD), lambda k: (0, 0)),
            pl.BlockSpec((1, 4, 256, 512), lambda k: (k, 0, 0, 0)),
        ),
        out_shape=(
            jax.ShapeDtypeStruct((528, HEAD), jnp.bfloat16),
            jax.ShapeDtypeStruct((2, 4, 256, 512), jnp.bfloat16),
        ),
        compiler_params=grant(12),
        name="project_keys_or_values",
    )(core, x, norm_gain, weights, gain, cosine, sine, extra)


def parcel_kernel(y_ref, own_ref, next_ref, far_ref, out_ref):
    for target in range(4):
        ahead = y_ref[0] <= target

        @pl.when(ahead)
        def _(target=target):
            out_ref[target, 0] = own_ref[...]
            out_ref[target, 1] = next_ref[...]

        @pl.when(jnp.logical_not(ahead))
        def _(target=target):
            out_ref[target, 0] = next_ref[...]
            out_ref[target, 1] = far_ref[...]


def parcels(y, own, next_plane, far_plane):
    vmem = pl.BlockSpec(memory_space=pltpu.VMEM)
    return pl.pallas_call(
        parcel_kernel,
        in_specs=[pl.BlockSpec(memory_space=pltpu.SMEM)] + [vmem] * 3,
        out_specs=vmem,
        out_shape=jax.ShapeDtypeStruct((4, 2, *own.shape), own.dtype),
        compiler_params=grant(4),
        name="parcels",
    )(y, own, next_plane, far_plane)


def window_kernel(y_ref, parts_ref, out_ref):
    for back in range(BACK + 1):
        place = BACK - back
        source = lax.rem(y_ref[0] + 4 - back % 4, 4)
        block = parts_ref[source, back // 4]
        out_ref[512 * place : 512 * (place + 1), :] = block[:512]
        out_ref[WINDOW + 16 * place : WINDOW + 16 * (place + 1), :] = block[512:]


def lay_window(y, parts):
    vmem = pl.BlockSpec(memory_space=pltpu.VMEM)
    return pl.pallas_call(
        window_kernel,
        in_specs=[pl.BlockSpec(memory_space=pltpu.SMEM), vmem],
        out_specs=vmem,
        out_shape=jax.ShapeDtypeStruct((WINDOW + 128, HEAD), jnp.bfloat16),
        compiler_params=grant(4),
        name="lay_window",
    )(y, parts)


def attention_kernel(
    core_ref,
    tokens_ref,
    gain_ref,
    cos_ref,
    sin_ref,
    own_ref,
    other_ref,
    wide_ref,
    here_ref,
    away_ref,
    x_ref,
    wq_ref,
    w_ref,
    token_sems,
    q_sems,
    kv_sems,
    out_sem,
    q_ref,
    kv_ref,
    tags_ref,
    reach_ref,
    m_ref,
    l_ref,
    acc_ref,
    attended_ref,
):
    tile = pl.program_id(0)
    lanes = lax.broadcasted_iota(jnp.int32, (1, TILE), 1)

    def query_copy(part):
        rows = pl.ds(part * 512, 512)
        return pltpu.make_async_copy(
            wide_ref.at[rows, pl.ds(0, 512)], wq_ref.at[rows, :], q_sems.at[part]
        )

    def token_copy(half):
        return pltpu.make_async_copy(tokens_ref.at[half], x_ref.at[half], token_sems.at[half])

    def out_copy():
        return pltpu.make_async_copy(wide_ref.at[:, pl.ds(512, 512)], w_ref, out_sem)

    own_copy = pltpu.make_async_copy(own_ref, kv_ref.at[core_ref[0]], kv_sems.at[0])
    other_copy = pltpu.make_async_copy(other_ref, kv_ref.at[1 - core_ref[0]], kv_sems.at[1])

    @pl.when(tile == 0)
    def _():
        token_copy(0).start()
        for part in range(4):
            query_copy(part).start()
        token_copy(1).start()
        own_copy.start()
        other_copy.start()
        out_copy().start()
        for part in range(4):
            query_copy(part).wait()
        for half in range(2):
            token_copy(half).wait()
            total = functools.reduce(
                jnp.add,
                [
                    jnp.dot(
                        x_ref[half, part],
                        wq_ref[part * 512 : (part + 1) * 512, :],
                        preferred_element_type=jnp.float32,
                    )
                    for part in range(4)
                ],
            )
            query_part(total, q_ref, half, gain_ref[...], cos_ref, sin_ref)
        own_copy.wait()
        other_copy.wait()
        for chip in range(BACK + 1):
            for core in range(2):
                row = WINDOW + 16 * chip
                extra = kv_ref[core, row : row + 16, :].astype(jnp.float32)
                place = 4 * chip + 2 * core
                tags_ref[place : place + 2, :] = extra[0:2]
                if chip == BACK:
                    reach_ref[core : core + 1, :] = extra[2:3]

    own_tile = 4 * BACK + tile
    doc_row = jnp.abs(tags_ref[pl.ds(own_tile, 1), :])
    diagonal = lax.broadcasted_iota(jnp.int32, (TILE, TILE), 0) == lax.broadcasted_iota(
        jnp.int32, (TILE, TILE), 1
    )
    query_doc = jnp.sum(jnp.where(diagonal, doc_row, 0.0), axis=1, keepdims=True)
    first_doc = jnp.sum(jnp.where(lanes == 0, doc_row, 0.0))
    before = jnp.sum(jnp.where(jnp.abs(tags_ref[...]) < first_doc, 1.0, 0.0)).astype(jnp.int32)
    reach_row = reach_ref[pl.ds(tile // 2, 1), :]
    reach = jnp.sum(jnp.where(lanes == tile % 2, reach_row, 0.0)).astype(jnp.int32)
    lowest = jnp.maximum(own_tile - reach, 0)
    first_tile = jnp.maximum(lowest, before // TILE)
    block_count = (own_tile - first_tile) // 4 + 1
    factor = math.log2(math.e) / math.sqrt(HEAD)
    query = q_ref[tile].reshape(4 * TILE, HEAD)
    wide_doc = jnp.broadcast_to(query_doc, (TILE, TILE))

    def scores_of(start_tile):
        start = pl.multiple_of(start_tile * TILE, TILE)
        return lax.dot_general(
            query,
            kv_ref[0, pl.ds(start, KEYS), :],
            (((1,), (1,)), ((), ())),
            preferred_element_type=jnp.float32,
        )

    def values_of(start_tile):
        return kv_ref[1, pl.ds(pl.multiple_of(start_tile * TILE, TILE), KEYS), :]

    def tags_of(start_tile, end_tile):
        rows = []
        for place in range(4):
            inside = (start_tile + place >= lowest) & (start_tile + place < end_tile)
            rows.append(jnp.where(inside, tags_ref[pl.ds(start_tile + place, 1), :], 0.0))
        return rows

    def lay_sums(pieces, peak):
        exps = [jnp.exp2(piece * factor - peak) for piece in pieces]
        return functools.reduce(jnp.add, exps), [piece.astype(jnp.bfloat16) for piece in exps]

    start_tile = own_tile - 3
    scores = scores_of(start_tile)
    tags = tags_of(start_tile, own_tile + 1)
    key_lane = lax.broadcasted_iota(jnp.int32, (TILE, TILE), 1)
    query_row = lax.broadcasted_iota(jnp.int32, (TILE, TILE), 0)
    visible = [wide_doc == tags[place] for place in range(4)]
    visible[3] = (visible[3] & (key_lane < query_row)) | diagonal
    weights = []
    for head in range(4):
        rows = slice(head * TILE, (head + 1) * TILE)
        pieces = [
            jnp.where(visible[place], scores[rows, place * TILE : (place + 1) * TILE], -1e30)
            for place in range(4)
        ]
        peak = jnp.max(functools.reduce(jnp.maximum, pieces), axis=1, keepdims=True) * factor
        peak = jnp.broadcast_to(peak, (TILE, HEAD))
        total, exps = lay_sums(pieces, peak)
        m_ref[rows, :] = peak
        l_ref[rows, :] = total
        weights.append(jnp.concatenate(exps, axis=1))
    acc_ref[...] = jnp.dot(
        jnp.concatenate(weights, axis=0), values_of(start_tile), preferred_element_type=jnp.float32
    )

    def one_block(block, carry):
        end_tile = own_tile + 1 - 4 * block
        start_tile = jnp.maximum(end_tile - 4, 0)
        scores = scores_of(start_tile)
        tags = tags_of(start_tile, end_tile)
        bias = [jnp.where(wide_doc == tags[place], 0.0, -1e30) for place in range(4)]
        weights, shrinks = [], []
        for head in range(4):
            rows = slice(head * TILE, (head + 1) * TILE)
            pieces = [
                scores[rows, place * TILE : (place + 1) * TILE] * factor + bias[place]
                for place in range(4)
            ]
            peak = jnp.max(functools.reduce(jnp.maximum, pieces), axis=1, keepdims=True)
            m_old = m_ref[rows, :]
            m_new = jnp.maximum(m_old, peak)
            exps = [jnp.exp2(piece - m_new) for piece in pieces]
            total = functools.reduce(jnp.add, exps)
            exps = [piece.astype(jnp.bfloat16) for piece in exps]
            shrink = jnp.exp2(m_old - m_new)
            m_ref[rows, :] = m_new
            l_ref[rows, :] = l_ref[rows, :] * shrink + total
            shrinks.append(shrink)
            weights.append(jnp.concatenate(exps, axis=1))
        mixed = jnp.dot(
            jnp.concatenate(weights, axis=0),
            values_of(start_tile),
            preferred_element_type=jnp.float32,
        )
        for head in range(4):
            rows = slice(head * TILE, (head + 1) * TILE)
            acc_ref[rows, :] = acc_ref[rows, :] * shrinks[head] + mixed[rows]
        return carry

    lax.fori_loop(1, block_count, one_block, 0)
    tile_rows = pl.ds(pl.multiple_of(tile * TILE, TILE), TILE)
    for head in range(4):
        rows = slice(head * TILE, (head + 1) * TILE)
        total = jnp.sum(l_ref[rows, :], axis=1, keepdims=True)
        attended_ref[tile_rows, head * HEAD : (head + 1) * HEAD] = (
            acc_ref[rows, :] / total
        ).astype(jnp.bfloat16)

    @pl.when(tile == 3)
    def _():
        out_copy().wait()
        here = pl.ds(pl.multiple_of(core_ref[0] * 256, 256), 256)
        away = pl.ds(pl.multiple_of((1 - core_ref[0]) * 256, 256), 256)
        both = jnp.concatenate([attended_ref[here, :], attended_ref[away, :]], axis=0)
        for part in range(4):
            sums = lax.dot_general(
                both,
                w_ref[part * 512 : (part + 1) * 512, :],
                (((1,), (1,)), ((), ())),
                preferred_element_type=jnp.float32,
            )
            here_ref[part] = sums[:256]
            away_ref[part] = sums[256:].astype(jnp.bfloat16)


def attend_and_project(core, x, gain, cosine, sine, own, other, wide):
    rows = WINDOW + 128
    return pl.pallas_call(
        attention_kernel,
        grid=(4,),
        in_specs=[
            pl.BlockSpec(memory_space=pltpu.SMEM),
            pl.BlockSpec(memory_space=pltpu.HBM),
            pl.BlockSpec((1, HEAD), lambda i: (0, 0)),
            pl.BlockSpec((512, HEAD // 2), lambda i: (0, 0)),
            pl.BlockSpec((512, HEAD // 2), lambda i: (0, 0)),
            pl.BlockSpec(memory_space=pltpu.HBM),
            pl.BlockSpec(memory_space=pltpu.HBM),
            pl.BlockSpec(memory_space=pltpu.HBM),
        ],
        out_specs=(
            pl.BlockSpec((4, 256, 512), lambda i: (0, 0, 0)),
            pl.BlockSpec((4, 256, 512), lambda i: (0, 0, 0)),
        ),
        out_shape=(
            jax.ShapeDtypeStruct((4, 256, 512), jnp.float32),
            jax.ShapeDtypeStruct((4, 256, 512), jnp.bfloat16),
        ),
        scratch_shapes=[
            pltpu.VMEM((2, 4, 256, 512), jnp.bfloat16),
            pltpu.VMEM((2048, 512), jnp.bfloat16),
            pltpu.VMEM((2048, 512), jnp.bfloat16),
            pltpu.SemaphoreType.DMA((2,)),
            pltpu.SemaphoreType.DMA((4,)),
            pltpu.SemaphoreType.DMA((2,)),
            pltpu.SemaphoreType.DMA,
            pltpu.VMEM((4, 4, TILE, HEAD), jnp.bfloat16),
            pltpu.VMEM((2, rows, HEAD), jnp.bfloat16),
            pltpu.VMEM((4 * (BACK + 1), TILE), jnp.float32),
            pltpu.VMEM((8, TILE), jnp.float32),
            pltpu.VMEM((4 * TILE, HEAD), jnp.float32),
            pltpu.VMEM((4 * TILE, HEAD), jnp.float32),
            pltpu.VMEM((4 * TILE, HEAD), jnp.float32),
            pltpu.VMEM((4 * TILE, 4 * HEAD), jnp.bfloat16),
        ],
        compiler_params=grant(32),
        name="attend_and_project",
    )(core, x, gain, cosine, sine, own, other, wide)


def layer(
    tokens,
    norm_gain,
    w_query,
    key_weight,
    value_weight,
    query_gain,
    key_gain,
    w_out,
    doc_ids,
    sentinel,
    tile_reach,
):
    core = lax.axis_index("core")
    core_arg = core.astype(jnp.int32).reshape(1)
    chip = lax.axis_index(CHIP)

    rows = [off_chip(rows) for rows in (w_query, w_out.T, key_weight, value_weight)]
    pieces = lay_pieces(*rows).reshape(8, 16, 1152)
    plane = lax.all_to_all(pieces, ("y", "core"), 0, 0, tiled=True).reshape(128, 1152)
    wide = lax.all_gather(plane[:, :1024], "z", axis=0, tiled=True)
    narrow = lax.all_gather(plane[:, 1024:], "z", axis=0, tiled=True)

    whole = copies(tokens, ("core", "head")).reshape(2, 4, 256, 512)

    positions = (chip * 512 + jnp.arange(512, dtype=jnp.int32)).astype(jnp.float32)
    freqs = THETA ** (-2.0 * jnp.arange(HEAD // 2, dtype=jnp.float32) / HEAD)
    angles = positions[:, None] * freqs[None, :]
    cosine, sine = jnp.cos(angles), jnp.sin(angles)

    tags = jnp.where(sentinel == 1, -(doc_ids + 1), doc_ids + 1).astype(jnp.bfloat16)
    extra = jnp.concatenate(
        [
            tags.reshape(2, TILE),
            jnp.pad(tile_reach.astype(jnp.bfloat16).reshape(1, 2), ((0, 0), (0, TILE - 2))),
            jnp.zeros((13, TILE), jnp.bfloat16),
        ]
    )
    own, normed = project_keys_or_values(
        core_arg,
        whole,
        norm_gain.reshape(4, 1, 512),
        narrow,
        key_gain.reshape(1, HEAD),
        cosine,
        sine,
        extra,
    )
    y_arg = lax.axis_index("y").astype(jnp.int32).reshape(1)
    next_plane, far_plane = (
        lax.ppermute(own, "z", [(source, source + step) for source in range(16 - step)])
        for step in (1, 2)
    )
    parts = parcels(y_arg, own, next_plane, far_plane)
    parts = lax.all_to_all(parts, "y", 0, 0, tiled=True)
    window = lay_window(y_arg, parts)
    window_other = lax.ppermute(window, "core", [(0, 1), (1, 0)])
    here, away = attend_and_project(
        core_arg,
        off_chip(normed),
        query_gain.reshape(1, HEAD),
        cosine,
        sine,
        off_chip(window),
        off_chip(window_other),
        off_chip(wide),
    )
    away = lax.ppermute(away, "core", [(0, 1), (1, 0)])
    partials = (here + away.astype(jnp.float32)).astype(jnp.bfloat16)
    shares = lax.all_to_all(partials, "head", 0, 0, tiled=True)
    return jnp.sum(shares.astype(jnp.float32), axis=0).astype(jnp.bfloat16)


def solution(mesh):
    split = Mesh(mesh.devices.reshape(16, 4, 2, 4), ("z", "y", "core", "head"))
    return jax.shard_map(
        layer,
        mesh=split,
        in_specs=(
            P(TOK, "head"),
            P(),
            P(TOK, "head"),
            P(TOK, "head"),
            P(TOK, "head"),
            P(),
            P(),
            P("head", TOK),
            P(TOK),
            P(TOK),
            P(TOK),
        ),
        out_specs=P(TOK, "head"),
        check_vma=False,
    )
```

```python
import functools
import math

import jax
import jax.numpy as jnp
from jax import lax
from jax.experimental import pallas as pl
from jax.experimental.pallas import tpu as pltpu
from jax.sharding import Mesh, PartitionSpec as P


HEAD = 128
TILE = 128
KEYS = 512
WINDOW = 4096
BACK = 7
EPSILON = 1e-06
THETA = 10000000.0
TOK = ("z", "y", "core")
CHIP = ("z", "y")


def grant(mebibytes):
    return pltpu.CompilerParams(vmem_limit_bytes=mebibytes << 20)


def off_chip(array):
    return pltpu.with_memory_space_constraint(array, pltpu.HBM)


def copies(shard, axis):
    count = lax.axis_size(axis)
    return lax.all_to_all(
        jnp.broadcast_to(shard[None], (count, *shard.shape)), axis, 0, 0, tiled=True
    )


def pieces_kernel(query_ref, out_ref_rows, key_ref, value_ref, pieces_ref):
    for y in range(4):
        for half in range(2):
            columns = slice(512 * half, 512 * (half + 1))
            pieces_ref[y, half, :, :512] = query_ref[:, columns]
            pieces_ref[y, half, :, 512:1024] = out_ref_rows[:, columns]
            pieces_ref[y, half, :, 1024:] = (key_ref, value_ref)[half][...]


def lay_pieces(query_rows, out_rows, key_rows, value_rows):
    vmem = pl.BlockSpec(memory_space=pltpu.VMEM)
    return pl.pallas_call(
        pieces_kernel,
        in_specs=[vmem] * 4,
        out_specs=vmem,
        out_shape=pltpu.VMEM((4, 2, 16, 1152), jnp.bfloat16),
        compiler_params=grant(4),
        name="lay_pieces",
    )(query_rows, out_rows, key_rows, value_rows)


def normed_and_turned(values, gain, cosine, sine):
    cosine = jnp.concatenate([cosine, cosine], axis=1)
    sine = jnp.concatenate([-sine, sine], axis=1)
    mean_square = jnp.mean(values * values, axis=-1, keepdims=True)
    scaled = values * lax.rsqrt(mean_square + EPSILON) * gain
    return scaled * cosine + pltpu.roll(scaled, HEAD // 2, 1) * sine


def query_part(total, q_ref, half, gain, cos_ref, sin_ref):
    for tile in range(2):
        rows = slice(tile * TILE, (tile + 1) * TILE)
        place = slice((2 * half + tile) * TILE, (2 * half + tile + 1) * TILE)
        for head in range(4):
            one = total[rows, head * HEAD : (head + 1) * HEAD]
            turned = normed_and_turned(one, gain, cos_ref[place, :], sin_ref[place, :])
            q_ref[2 * half + tile, head] = turned.astype(jnp.bfloat16)


def key_value_kernel(
    core_ref, x_ref, norm_ref, w_ref, gain_ref, cos_ref, sin_ref, extra_ref, out_ref, normed_ref
):
    rows = pl.ds(pl.multiple_of(pl.program_id(0) * 256, 256), 256)
    parts = [x_ref[0, part].astype(jnp.float32) for part in range(4)]
    squares = functools.reduce(jnp.add, [part * part for part in parts])
    level = lax.rsqrt(jnp.sum(squares, axis=1, keepdims=True) / 2048 + EPSILON)
    products = []
    for part in range(4):
        normed = (parts[part] * level * norm_ref[part]).astype(jnp.bfloat16)
        normed_ref[0, part] = normed
        products.append(
            jnp.dot(
                normed,
                w_ref[part * 512 : (part + 1) * 512, :],
                preferred_element_type=jnp.float32,
            )
        )
    total = functools.reduce(jnp.add, products)
    turned = normed_and_turned(total, gain_ref[...], cos_ref[...], sin_ref[...])
    out_ref[rows, :] = jnp.where(core_ref[0] == 0, turned, total).astype(jnp.bfloat16)

    @pl.when(pl.program_id(0) == 0)
    def _():
        out_ref[512:528, :] = extra_ref[...]


def project_keys_or_values(core, x, norm_gain, weights, gain, cosine, sine, extra):
    return pl.pallas_call(
        key_value_kernel,
        grid=(2,),
        in_specs=[
            pl.BlockSpec(memory_space=pltpu.SMEM),
            pl.BlockSpec((1, 4, 256, 512), lambda k: (k, 0, 0, 0)),
            pl.BlockSpec((4, 1, 512), lambda k: (0, 0, 0)),
            pl.BlockSpec((2048, HEAD), lambda k: (0, 0)),
            pl.BlockSpec((1, HEAD), lambda k: (0, 0)),
            pl.BlockSpec((256, HEAD // 2), lambda k: (k, 0)),
            pl.BlockSpec((256, HEAD // 2), lambda k: (k, 0)),
            pl.BlockSpec((16, HEAD), lambda k: (0, 0)),
        ],
        out_specs=(
            pl.BlockSpec((528, HEAD), lambda k: (0, 0)),
            pl.BlockSpec((1, 4, 256, 512), lambda k: (k, 0, 0, 0)),
        ),
        out_shape=(
            jax.ShapeDtypeStruct((528, HEAD), jnp.bfloat16),
            jax.ShapeDtypeStruct((2, 4, 256, 512), jnp.bfloat16),
        ),
        compiler_params=grant(12),
        name="project_keys_or_values",
    )(core, x, norm_gain, weights, gain, cosine, sine, extra)


def parcel_kernel(y_ref, own_ref, next_ref, far_ref, out_ref):
    for target in range(4):
        ahead = y_ref[0] <= target

        @pl.when(ahead)
        def _(target=target):
            out_ref[target, 0] = own_ref[...]
            out_ref[target, 1] = next_ref[...]

        @pl.when(jnp.logical_not(ahead))
        def _(target=target):
            out_ref[target, 0] = next_ref[...]
            out_ref[target, 1] = far_ref[...]


def parcels(y, own, next_plane, far_plane):
    vmem = pl.BlockSpec(memory_space=pltpu.VMEM)
    return pl.pallas_call(
        parcel_kernel,
        in_specs=[pl.BlockSpec(memory_space=pltpu.SMEM)] + [vmem] * 3,
        out_specs=vmem,
        out_shape=jax.ShapeDtypeStruct((4, 2, *own.shape), own.dtype),
        compiler_params=grant(4),
        name="parcels",
    )(y, own, next_plane, far_plane)


def window_kernel(y_ref, parts_ref, out_ref):
    for back in range(BACK + 1):
        place = BACK - back
        source = lax.rem(y_ref[0] + 4 - back % 4, 4)
        block = parts_ref[source, back // 4]
        out_ref[512 * place : 512 * (place + 1), :] = block[:512]
        out_ref[WINDOW + 16 * place : WINDOW + 16 * (place + 1), :] = block[512:]


def lay_window(y, parts):
    vmem = pl.BlockSpec(memory_space=pltpu.VMEM)
    return pl.pallas_call(
        window_kernel,
        in_specs=[pl.BlockSpec(memory_space=pltpu.SMEM), vmem],
        out_specs=vmem,
        out_shape=jax.ShapeDtypeStruct((WINDOW + 128, HEAD), jnp.bfloat16),
        compiler_params=grant(4),
        name="lay_window",
    )(y, parts)


def attention_kernel(
    core_ref,
    tokens_ref,
    gain_ref,
    cos_ref,
    sin_ref,
    own_ref,
    other_ref,
    wide_ref,
    here_ref,
    away_ref,
    x_ref,
    wq_ref,
    w_ref,
    token_sems,
    q_sems,
    kv_sems,
    out_sem,
    q_ref,
    kv_ref,
    tags_ref,
    reach_ref,
    m_ref,
    l_ref,
    acc_ref,
    attended_ref,
):
    tile = pl.program_id(0)
    lanes = lax.broadcasted_iota(jnp.int32, (1, TILE), 1)

    def query_copy(part):
        rows = pl.ds(part * 512, 512)
        return pltpu.make_async_copy(
            wide_ref.at[rows, pl.ds(0, 512)], wq_ref.at[rows, :], q_sems.at[part]
        )

    def token_copy(half):
        return pltpu.make_async_copy(tokens_ref.at[half], x_ref.at[half], token_sems.at[half])

    def out_copy():
        return pltpu.make_async_copy(wide_ref.at[:, pl.ds(512, 512)], w_ref, out_sem)

    own_copy = pltpu.make_async_copy(own_ref, kv_ref.at[core_ref[0]], kv_sems.at[0])
    other_copy = pltpu.make_async_copy(other_ref, kv_ref.at[1 - core_ref[0]], kv_sems.at[1])

    @pl.when(tile == 0)
    def _():
        token_copy(0).start()
        for part in range(4):
            query_copy(part).start()
        token_copy(1).start()
        own_copy.start()
        other_copy.start()
        out_copy().start()
        for part in range(4):
            query_copy(part).wait()
        for half in range(2):
            token_copy(half).wait()
            total = functools.reduce(
                jnp.add,
                [
                    jnp.dot(
                        x_ref[half, part],
                        wq_ref[part * 512 : (part + 1) * 512, :],
                        preferred_element_type=jnp.float32,
                    )
                    for part in range(4)
                ],
            )
            query_part(total, q_ref, half, gain_ref[...], cos_ref, sin_ref)
        own_copy.wait()
        other_copy.wait()
        for chip in range(BACK + 1):
            for core in range(2):
                row = WINDOW + 16 * chip
                extra = kv_ref[core, row : row + 16, :].astype(jnp.float32)
                place = 4 * chip + 2 * core
                tags_ref[place : place + 2, :] = extra[0:2]
                if chip == BACK:
                    reach_ref[core : core + 1, :] = extra[2:3]

    own_tile = 4 * BACK + tile
    doc_row = jnp.abs(tags_ref[pl.ds(own_tile, 1), :])
    diagonal = lax.broadcasted_iota(jnp.int32, (TILE, TILE), 0) == lax.broadcasted_iota(
        jnp.int32, (TILE, TILE), 1
    )
    query_doc = jnp.sum(jnp.where(diagonal, doc_row, 0.0), axis=1, keepdims=True)
    first_doc = jnp.sum(jnp.where(lanes == 0, doc_row, 0.0))
    before = jnp.sum(jnp.where(jnp.abs(tags_ref[...]) < first_doc, 1.0, 0.0)).astype(jnp.int32)
    reach_row = reach_ref[pl.ds(tile // 2, 1), :]
    reach = jnp.sum(jnp.where(lanes == tile % 2, reach_row, 0.0)).astype(jnp.int32)
    lowest = jnp.maximum(own_tile - reach, 0)
    first_tile = jnp.maximum(lowest, before // TILE)
    block_count = (own_tile - first_tile) // 4 + 1
    factor = math.log2(math.e) / math.sqrt(HEAD)
    query = q_ref[tile].reshape(4 * TILE, HEAD)
    wide_doc = jnp.broadcast_to(query_doc, (TILE, TILE))

    def scores_of(start_tile):
        start = pl.multiple_of(start_tile * TILE, TILE)
        return lax.dot_general(
            query,
            kv_ref[0, pl.ds(start, KEYS), :],
            (((1,), (1,)), ((), ())),
            preferred_element_type=jnp.float32,
        )

    def values_of(start_tile):
        return kv_ref[1, pl.ds(pl.multiple_of(start_tile * TILE, TILE), KEYS), :]

    def tags_of(start_tile, end_tile):
        rows = []
        for place in range(4):
            inside = (start_tile + place >= lowest) & (start_tile + place < end_tile)
            rows.append(jnp.where(inside, tags_ref[pl.ds(start_tile + place, 1), :], 0.0))
        return rows

    def lay_sums(pieces, peak):
        exps = [jnp.exp2(piece * factor - peak) for piece in pieces]
        return functools.reduce(jnp.add, exps), [piece.astype(jnp.bfloat16) for piece in exps]

    start_tile = own_tile - 3
    scores = scores_of(start_tile)
    tags = tags_of(start_tile, own_tile + 1)
    key_lane = lax.broadcasted_iota(jnp.int32, (TILE, TILE), 1)
    query_row = lax.broadcasted_iota(jnp.int32, (TILE, TILE), 0)
    visible = [wide_doc == tags[place] for place in range(4)]
    visible[3] = (visible[3] & (key_lane < query_row)) | diagonal
    weights = []
    for head in range(4):
        rows = slice(head * TILE, (head + 1) * TILE)
        pieces = [
            jnp.where(visible[place], scores[rows, place * TILE : (place + 1) * TILE], -1e30)
            for place in range(4)
        ]
        peak = jnp.max(functools.reduce(jnp.maximum, pieces), axis=1, keepdims=True) * factor
        peak = jnp.broadcast_to(peak, (TILE, HEAD))
        total, exps = lay_sums(pieces, peak)
        m_ref[rows, :] = peak
        l_ref[rows, :] = total
        weights.append(jnp.concatenate(exps, axis=1))
    acc_ref[...] = jnp.dot(
        jnp.concatenate(weights, axis=0), values_of(start_tile), preferred_element_type=jnp.float32
    )

    def one_block(block, carry):
        end_tile = own_tile + 1 - 4 * block
        start_tile = jnp.maximum(end_tile - 4, 0)
        scores = scores_of(start_tile)
        tags = tags_of(start_tile, end_tile)
        bias = [jnp.where(wide_doc == tags[place], 0.0, -1e30) for place in range(4)]
        weights, shrinks = [], []
        for head in range(4):
            rows = slice(head * TILE, (head + 1) * TILE)
            pieces = [
                scores[rows, place * TILE : (place + 1) * TILE] * factor + bias[place]
                for place in range(4)
            ]
            peak = jnp.max(functools.reduce(jnp.maximum, pieces), axis=1, keepdims=True)
            m_old = m_ref[rows, :]
            m_new = jnp.maximum(m_old, peak)
            exps = [jnp.exp2(piece - m_new) for piece in pieces]
            total = functools.reduce(jnp.add, exps)
            exps = [piece.astype(jnp.bfloat16) for piece in exps]
            shrink = jnp.exp2(m_old - m_new)
            m_ref[rows, :] = m_new
            l_ref[rows, :] = l_ref[rows, :] * shrink + total
            shrinks.append(shrink)
            weights.append(jnp.concatenate(exps, axis=1))
        mixed = jnp.dot(
            jnp.concatenate(weights, axis=0),
            values_of(start_tile),
            preferred_element_type=jnp.float32,
        )
        for head in range(4):
            rows = slice(head * TILE, (head + 1) * TILE)
            acc_ref[rows, :] = acc_ref[rows, :] * shrinks[head] + mixed[rows]
        return carry

    lax.fori_loop(1, block_count, one_block, 0)
    tile_rows = pl.ds(pl.multiple_of(tile * TILE, TILE), TILE)
    for head in range(4):
        rows = slice(head * TILE, (head + 1) * TILE)
        total = jnp.sum(l_ref[rows, :], axis=1, keepdims=True)
        attended_ref[tile_rows, head * HEAD : (head + 1) * HEAD] = (
            acc_ref[rows, :] / total
        ).astype(jnp.bfloat16)

    @pl.when(tile == 3)
    def _():
        out_copy().wait()
        here = pl.ds(pl.multiple_of(core_ref[0] * 256, 256), 256)
        away = pl.ds(pl.multiple_of((1 - core_ref[0]) * 256, 256), 256)
        both = jnp.concatenate([attended_ref[here, :], attended_ref[away, :]], axis=0)
        for part in range(4):
            sums = lax.dot_general(
                both,
                w_ref[part * 512 : (part + 1) * 512, :],
                (((1,), (1,)), ((), ())),
                preferred_element_type=jnp.float32,
            )
            here_ref[part] = sums[:256]
            away_ref[part] = sums[256:].astype(jnp.bfloat16)


def attend_and_project(core, x, gain, cosine, sine, own, other, wide):
    rows = WINDOW + 128
    return pl.pallas_call(
        attention_kernel,
        grid=(4,),
        in_specs=[
            pl.BlockSpec(memory_space=pltpu.SMEM),
            pl.BlockSpec(memory_space=pltpu.HBM),
            pl.BlockSpec((1, HEAD), lambda i: (0, 0)),
            pl.BlockSpec((512, HEAD // 2), lambda i: (0, 0)),
            pl.BlockSpec((512, HEAD // 2), lambda i: (0, 0)),
            pl.BlockSpec(memory_space=pltpu.HBM),
            pl.BlockSpec(memory_space=pltpu.HBM),
            pl.BlockSpec(memory_space=pltpu.HBM),
        ],
        out_specs=(
            pl.BlockSpec((4, 256, 512), lambda i: (0, 0, 0)),
            pl.BlockSpec((4, 256, 512), lambda i: (0, 0, 0)),
        ),
        out_shape=(
            jax.ShapeDtypeStruct((4, 256, 512), jnp.float32),
            jax.ShapeDtypeStruct((4, 256, 512), jnp.bfloat16),
        ),
        scratch_shapes=[
            pltpu.VMEM((2, 4, 256, 512), jnp.bfloat16),
            pltpu.VMEM((2048, 512), jnp.bfloat16),
            pltpu.VMEM((2048, 512), jnp.bfloat16),
            pltpu.SemaphoreType.DMA((2,)),
            pltpu.SemaphoreType.DMA((4,)),
            pltpu.SemaphoreType.DMA((2,)),
            pltpu.SemaphoreType.DMA,
            pltpu.VMEM((4, 4, TILE, HEAD), jnp.bfloat16),
            pltpu.VMEM((2, rows, HEAD), jnp.bfloat16),
            pltpu.VMEM((4 * (BACK + 1), TILE), jnp.float32),
            pltpu.VMEM((8, TILE), jnp.float32),
            pltpu.VMEM((4 * TILE, HEAD), jnp.float32),
            pltpu.VMEM((4 * TILE, HEAD), jnp.float32),
            pltpu.VMEM((4 * TILE, HEAD), jnp.float32),
            pltpu.VMEM((4 * TILE, 4 * HEAD), jnp.bfloat16),
        ],
        compiler_params=grant(32),
        name="attend_and_project",
    )(core, x, gain, cosine, sine, own, other, wide)


def layer(
    tokens,
    norm_gain,
    w_query,
    key_weight,
    value_weight,
    query_gain,
    key_gain,
    w_out,
    doc_ids,
    sentinel,
    tile_reach,
):
    core = lax.axis_index("core")
    core_arg = core.astype(jnp.int32).reshape(1)
    chip = lax.axis_index(CHIP)

    rows = [off_chip(rows) for rows in (w_query, w_out.T, key_weight, value_weight)]
    pieces = lay_pieces(*rows).reshape(8, 16, 1152)
    plane = lax.all_to_all(pieces, ("y", "core"), 0, 0, tiled=True).reshape(128, 1152)
    wide = lax.all_gather(plane[:, :1024], "z", axis=0, tiled=True)
    narrow = lax.all_gather(plane[:, 1024:], "z", axis=0, tiled=True)

    whole = copies(tokens, ("core", "head")).reshape(2, 4, 256, 512)

    positions = (chip * 512 + jnp.arange(512, dtype=jnp.int32)).astype(jnp.float32)
    freqs = THETA ** (-2.0 * jnp.arange(HEAD // 2, dtype=jnp.float32) / HEAD)
    angles = positions[:, None] * freqs[None, :]
    cosine, sine = jnp.cos(angles), jnp.sin(angles)

    tags = jnp.where(sentinel == 1, -(doc_ids + 1), doc_ids + 1).astype(jnp.bfloat16)
    extra = jnp.concatenate(
        [
            tags.reshape(2, TILE),
            jnp.pad(tile_reach.astype(jnp.bfloat16).reshape(1, 2), ((0, 0), (0, TILE - 2))),
            jnp.zeros((13, TILE), jnp.bfloat16),
        ]
    )
    own, normed = project_keys_or_values(
        core_arg,
        whole,
        norm_gain.reshape(4, 1, 512),
        narrow,
        key_gain.reshape(1, HEAD),
        cosine,
        sine,
        extra,
    )
    y_arg = lax.axis_index("y").astype(jnp.int32).reshape(1)
    ahead = [(source, source + 1) for source in range(15)]
    next_plane = lax.ppermute(own, "z", ahead)
    far_plane = lax.ppermute(next_plane, "z", ahead)
    parts = parcels(y_arg, own, next_plane, far_plane)
    parts = lax.all_to_all(parts, "y", 0, 0, tiled=True)
    window = lay_window(y_arg, parts)
    window_other = lax.ppermute(window, "core", [(0, 1), (1, 0)])
    here, away = attend_and_project(
        core_arg,
        off_chip(normed),
        query_gain.reshape(1, HEAD),
        cosine,
        sine,
        off_chip(window),
        off_chip(window_other),
        off_chip(wide),
    )
    away = lax.ppermute(away, "core", [(0, 1), (1, 0)])
    partials = (here + away.astype(jnp.float32)).astype(jnp.bfloat16)
    shares = lax.all_to_all(partials, "head", 0, 0, tiled=True)
    return jnp.sum(shares.astype(jnp.float32), axis=0).astype(jnp.bfloat16)


def solution(mesh):
    split = Mesh(mesh.devices.reshape(16, 4, 2, 4), ("z", "y", "core", "head"))
    return jax.shard_map(
        layer,
        mesh=split,
        in_specs=(
            P(TOK, "head"),
            P(),
            P(TOK, "head"),
            P(TOK, "head"),
            P(TOK, "head"),
            P(),
            P(),
            P("head", TOK),
            P(TOK),
            P(TOK),
            P(TOK),
        ),
        out_specs=P(TOK, "head"),
        check_vma=False,
    )
```
